256 devices in a mesh: seg: 8 (over x_hi, y), lat: 32 (over z, x_lo, core).
Axes of the slice: x: 4 (x_hi: 2, x_lo: 2; x = x_hi * 2 + x_lo), y: 4, z: 8, core: 2. Of those that a mesh axis runs over, the one named last changes fastest.
Arguments:
- coh_map: bfloat16 [8, 65536, 128], P('seg', 'lat'), may hold values from 0 to 40, as said below
- positions: int32 [8, 4096], P('seg', 'lat'), may hold values from 0 to 16776959, as said below
- counts: int32 [64], P('lat'), may hold values from 1 to 64, as said below
Outputs:
- semi_stat: bfloat16 [4096, 128], P('lat')
- excess: float32 [64, 128], P('lat')
The draws below stay inside these ranges and needn't reach their ends.
Inputs may be any that keep to these rules, and one draw needn't show every extreme that they name: `coh_map`: nonnegative. `counts`: the first block has 1 valid point and the last block 64. `positions`: the bins are split into 32 aligned slices of 2048 bins; a point's two bins lie in the same slice; in each segment, at most 8 of the 128 points of one index of lat have their bins in one slice, and that most is reached in every draw.
All inputs are finite; a program needn't handle non-finite values.
Results may differ from the reference program's by a relative error of at most 0.001.
Values sent between devices are 32-bit elements; how exact they have to be, the bound alone decides.
A program may use at most 64 MiB of HBM per device.

```python
import math
import jax
import jax.numpy as jnp
from jax import lax

F = 65536
NSD = 128
BLK = 64
PT_DEV = 128
S = 8
NB = 64
SLICE = 2048
N_LAT = 32


def draw_coh_map(key, part):
    first_key, second_key, third_key = jax.random.split(jax.random.fold_in(key, 11), 3)
    column_scale = jnp.exp(jax.random.uniform(third_key, (NSD,), jnp.float32, math.log(0.1), 0.0))
    values = 2.0 * (jax.random.exponential(first_key, (S, F, NSD), jnp.float32) + jax.random.exponential(second_key, (S, F, NSD), jnp.float32))
    return jnp.clip(values * column_scale, 0.0, 40.0).astype(jnp.bfloat16)


def draw_positions(key, part):
    base_key = jax.random.fold_in(key, 37)
    perm_key, split_key, shuffle_key, bin_key, frac_key = jax.random.split(base_key, 5)
    pair_total = N_LAT // 2
    slot_limit = 2 * PT_DEV // N_LAT
    dest_scores = jax.random.randint(perm_key, (S, N_LAT, N_LAT), 0, 1 << 20, dtype=jnp.int32) * N_LAT + jnp.arange(N_LAT, dtype=jnp.int32)
    dest_perm = jnp.argsort(dest_scores, axis=-1, stable=True).astype(jnp.int32)
    split_at = jax.random.randint(split_key, (S, N_LAT, pair_total), 0, slot_limit + 1, dtype=jnp.int32)
    split_at = split_at.at[:, :, 0].set(slot_limit)
    point_ids = jnp.arange(PT_DEV, dtype=jnp.int32)
    pair_ids = point_ids // slot_limit
    within = point_ids % slot_limit
    split_points = jnp.take(split_at, pair_ids, axis=2)
    first_dest = jnp.take(dest_perm, 2 * pair_ids, axis=2)
    second_dest = jnp.take(dest_perm, 2 * pair_ids + 1, axis=2)
    dest = jnp.where(within[None, None, :] < split_points, first_dest, second_dest)
    point_scores = jax.random.randint(shuffle_key, (S, N_LAT, PT_DEV), 0, 1 << 20, dtype=jnp.int32) * PT_DEV + point_ids
    shuffle = jnp.argsort(point_scores, axis=-1, stable=True).astype(jnp.int32)
    dest = jnp.take_along_axis(dest, shuffle, axis=-1)
    low_bin = dest * SLICE + jax.random.randint(bin_key, (S, N_LAT, PT_DEV), 0, SLICE - 1, dtype=jnp.int32)
    drawn = low_bin * 256 + jax.random.randint(frac_key, (S, N_LAT, PT_DEV), 0, 256, dtype=jnp.int32)
    return drawn.reshape(S, N_LAT * PT_DEV).astype(jnp.int32)


def draw_counts(key, part):
    block_id = jnp.arange(NB, dtype=jnp.int32)
    low_bound = 1 + BLK // 2 * block_id // NB
    high_bound = 1 + BLK // 4 + 3 * BLK // 4 * block_id // NB
    raw_bits = jax.random.randint(jax.random.fold_in(key, 23), (NB,), 0, 1 << 20, dtype=jnp.int32)
    drawn = low_bound + raw_bits % (high_bound - low_bound)
    drawn = drawn.at[0].set(1).at[NB - 1].set(BLK)
    return drawn.astype(jnp.int32)


def setup_inputs(seed: int = 0) -> dict:
    key_list = jax.random.split(jax.random.key(seed), 4)
    coh_map = draw_coh_map(jax.random.fold_in(key_list[3], 71), 0)
    positions = draw_positions(jax.random.fold_in(key_list[3], 71), 0)
    counts = draw_counts(jax.random.fold_in(key_list[3], 71), 0)
    return {"coh_map": coh_map, "positions": positions, "counts": counts}


def reference(coh_map, positions, counts):
    low_bin = positions // 256
    fraction = (positions % 256).astype(jnp.float32) / 256.0

    def accumulate(running, inputs):
        seg_map, low_index, weight_hi = inputs
        near_rows = jnp.take(seg_map, low_index, axis=0).astype(jnp.float32)
        far_rows = jnp.take(seg_map, low_index + 1, axis=0).astype(jnp.float32)
        running = running + (1.0 - weight_hi)[:, None] * near_rows + weight_hi[:, None] * far_rows
        return running, None

    start_sum = jnp.zeros((positions.shape[1], coh_map.shape[2]), jnp.float32)
    summed, _ = lax.scan(accumulate, start_sum, (coh_map, low_bin, fraction))
    semi_stat = summed / coh_map.shape[0]
    grouped = semi_stat.reshape(NB, BLK, NSD)
    slot_index = lax.broadcasted_iota(jnp.int32, (NB, BLK, 1), 1)
    live_mask = slot_index < counts[:, None, None]
    block_sum = jnp.sum(jnp.where(live_mask, grouped, 0.0), axis=1)
    count_float = counts.astype(jnp.float32)
    block_mean = block_sum / count_float[:, None]
    global_mean = jnp.sum(block_sum, axis=0) / jnp.sum(count_float)
    excess = block_mean - global_mean[None, :]
    return semi_stat.astype(jnp.bfloat16), excess
```

```python
import functools

import jax
import jax.numpy as jnp
from jax import lax
from jax.experimental import pallas as pl
from jax.experimental.pallas import tpu as pltpu
from jax.sharding import PartitionSpec as P

MESH = pl.DeviceIdType.MESH
PER_BIN = 256
SUB = 4
PAIR = 2
LIVE = 4.0
VALID = 4096.0


def wait_bytes(ref, sem):
    pltpu.make_async_copy(ref, ref, sem).wait()


def kernel(
    n_seg,
    n_lat,
    map_ref,
    pos_ref,
    cnt_ref,
    stat_ref,
    exc_ref,
    table,
    note,
    heard,
    pair_note,
    rows_out,
    rows_in,
    pick,
    part,
    table_sem,
    note_send,
    heard_sem,
    pair_sem,
    rows_send,
    rows_sem,
    part_send,
    part_sem,
):
    n_y = n_seg // PAIR
    n_z = n_lat // SUB
    bins, width = table.shape
    points = pos_ref.shape[1]
    blocks = exc_ref.shape[0]
    block_size = points // blocks
    slots = 2 * points // n_lat
    span = bins * PER_BIN
    f32, bf16, i32 = jnp.float32, jnp.bfloat16, jnp.int32

    seg = lax.axis_index("seg")
    lat = lax.axis_index("lat")
    group, y = seg // n_y, seg % n_y
    other_seg = (PAIR - 1 - group) * n_y + y
    z, q = lat // SUB, lat % SUB

    def lat_at(t):
        g, s = t // SUB, t % SUB
        odd = g % 2
        dz = n_z // 2 + (1 - odd) * (g // 2) - odd * ((g + 1) // 2)
        return ((z + dz) % n_z) * SUB + (q + s + 1) % SUB

    load = pltpu.make_async_copy(map_ref.at[0], table, table_sem)
    load.start()

    barrier = pltpu.get_barrier_semaphore()

    def greet(t, _):
        d = lat_at(t)
        pl.semaphore_signal(barrier, inc=1, device_id=(seg, d), device_id_type=MESH)
        pl.semaphore_signal(barrier, inc=1, device_id=(other_seg, d), device_id_type=MESH)
        return _

    lax.fori_loop(0, n_lat - 1, greet, 0)
    pl.semaphore_signal(barrier, inc=1, device_id=(other_seg, lat), device_id_type=MESH)
    for k in range(1, n_y):
        peer = group * n_y + (y + k) % n_y
        pl.semaphore_signal(barrier, inc=1, device_id=(peer, lat), device_id_type=MESH)

    lane = lax.broadcasted_iota(i32, (1, points), 1)
    limit = jnp.zeros((1, points), i32)
    for b in range(blocks):
        limit = jnp.where(lane // block_size == b, cnt_ref[b] + b * block_size, limit)
    note[0:1, :] = pos_ref[...]
    note[1:2, :] = jnp.where(lane < limit, 1, 0)

    pl.semaphore_wait(barrier, 2 * n_lat - 1 + n_y - 1)

    def tell(t, _):
        pltpu.make_async_remote_copy(
            src_ref=note,
            dst_ref=heard.at[lat],
            send_sem=note_send,
            recv_sem=heard_sem,
            device_id=(seg, lat_at(t)),
            device_id_type=MESH,
        ).start()
        return _

    lax.fori_loop(0, n_lat - 1, tell, 0)
    pltpu.make_async_remote_copy(
        src_ref=note,
        dst_ref=pair_note,
        send_sem=note_send,
        recv_sem=pair_sem,
        device_id=(other_seg, lat),
        device_id_type=MESH,
    ).start()
    pltpu.make_async_copy(note, heard.at[lat], heard_sem).start()

    before_mat = jnp.where(
        lax.broadcasted_iota(i32, (points, points), 0)
        < lax.broadcasted_iota(i32, (points, points), 1),
        1.0,
        0.0,
    ).astype(bf16)

    load.wait()
    wait_bytes(heard, heard_sem)

    pos = heard[:, 0, :]
    ok = heard[:, 1, :]
    rel = pos - lat * span
    hit = (rel >= 0) & (rel < span)
    before = jnp.dot(
        jnp.where(hit, 1.0, 0.0).astype(bf16), before_mat, preferred_element_type=f32
    )
    key = jnp.where(hit, before, -1.0)
    coded = jnp.where(hit, rel.astype(f32) * (1.0 / PER_BIN) + LIVE + ok.astype(f32) * VALID, 0.0)
    slot_id = lax.broadcasted_iota(i32, (n_lat, slots, points), 1).astype(f32)
    chosen = jnp.where(key[:, None, :] == slot_id, coded[:, None, :], 0.0)
    code = jnp.sum(chosen, axis=2, keepdims=True).reshape(n_lat * slots, 1)
    is_valid = code >= VALID
    where_ = code - jnp.where(is_valid, VALID + LIVE, LIVE)
    bin_id = lax.broadcasted_iota(i32, (1, bins), 1).astype(f32)
    weights = jnp.maximum(1.0 - jnp.abs(where_ - bin_id), 0.0).astype(bf16)
    rows = jnp.dot(weights, table[...], preferred_element_type=f32)
    valid_sum = jnp.sum(jnp.where(is_valid, rows, 0.0), axis=0, keepdims=True)
    rows_out[:, 0:slots, :] = rows.reshape(n_lat, slots, width)
    rows_out[:, slots : slots + 1, :] = jnp.broadcast_to(valid_sum[None], (n_lat, 1, width))

    def give(t, _):
        d = lat_at(t)
        pltpu.make_async_remote_copy(
            src_ref=rows_out.at[d],
            dst_ref=rows_in.at[group, lat],
            send_sem=rows_send.at[1],
            recv_sem=rows_sem.at[group],
            device_id=(other_seg, d),
            device_id_type=MESH,
        ).start()
        pltpu.make_async_remote_copy(
            src_ref=rows_out.at[d],
            dst_ref=rows_in.at[group, lat],
            send_sem=rows_send.at[0],
            recv_sem=rows_sem.at[group],
            device_id=(seg, d),
            device_id_type=MESH,
        ).start()
        return _

    lax.fori_loop(0, n_lat - 1, give, 0)
    pltpu.make_async_remote_copy(
        src_ref=rows_out.at[lat],
        dst_ref=rows_in.at[group, lat],
        send_sem=rows_send.at[1],
        recv_sem=rows_sem.at[group],
        device_id=(other_seg, lat),
        device_id_type=MESH,
    ).start()
    pltpu.make_async_copy(rows_out.at[lat], rows_in.at[group, lat], rows_sem.at[group]).start()

    wait_bytes(pair_note, pair_sem)
    dest_id = lax.broadcasted_iota(i32, (n_lat, points), 0)
    flat_id = lax.broadcasted_iota(i32, (n_lat * slots, points), 0).astype(f32)
    for g in range(PAIR):
        mine = jnp.where(group == g, note[0:1, :], pair_note[0:1, :])
        dest = mine // span
        at_dest = jnp.where(dest == dest_id, 1.0, 0.0)
        ahead = jnp.dot(at_dest.astype(bf16), before_mat, preferred_element_type=f32)
        slot = jnp.sum(at_dest * ahead, axis=0, keepdims=True)
        flat = dest.astype(f32) * slots + slot
        choice = jnp.where(flat_id == flat, 1.0, 0.0)
        pick[:, g * n_lat * slots : (g + 1) * n_lat * slots] = choice.T.astype(bf16)
    total_count = jnp.sum(ok.astype(f32))

    for g in range(PAIR):
        wait_bytes(rows_in.at[g], rows_sem.at[g])
    got = rows_in[:, :, 0:slots, :].reshape(PAIR * n_lat * slots, width)
    high = got.astype(bf16)
    rest = got - high.astype(f32)
    mid = rest.astype(bf16)
    low = (rest - mid.astype(f32)).astype(bf16)
    chooser = pick[...]
    own = (
        jnp.dot(chooser, low, preferred_element_type=f32)
        + jnp.dot(chooser, mid, preferred_element_type=f32)
        + jnp.dot(chooser, high, preferred_element_type=f32)
    )
    part[y, 0:points, :] = own
    sums = rows_in[:, :, slots, :].reshape(PAIR * n_lat, width)
    part[y, points : points + 8, :] = jnp.broadcast_to(
        jnp.sum(sums, axis=0, keepdims=True), (8, width)
    )

    for k in range(1, n_y):
        peer = group * n_y + (y + k % (n_y - 1) + 1) % n_y
        pltpu.make_async_remote_copy(
            src_ref=part.at[y],
            dst_ref=part.at[y],
            send_sem=part_send,
            recv_sem=part_sem,
            device_id=(peer, lat),
            device_id_type=MESH,
        ).start()
    wait_bytes(part.at[0 : n_y - 1], part_sem)

    all_sum = part[0]
    for k in range(1, n_y):
        all_sum = all_sum + part[k]
    stat = all_sum[0:points] * (1.0 / n_seg)
    stat_ref[...] = stat.astype(bf16)
    global_mean = all_sum[points : points + 1] * (1.0 / n_seg) / total_count
    row_id = lax.broadcasted_iota(i32, (block_size, width), 0)
    for b in range(blocks):
        count = cnt_ref[b]
        block = stat[b * block_size : (b + 1) * block_size]
        block_sum = jnp.sum(jnp.where(row_id < count, block, 0.0), axis=0, keepdims=True)
        exc_ref[b : b + 1, :] = block_sum / count.astype(f32) - global_mean

    wait_bytes(heard, note_send)
    wait_bytes(rows_in.at[0, 0 : n_lat - 1], rows_send.at[0])
    wait_bytes(rows_in.at[0], rows_send.at[1])
    wait_bytes(part.at[0 : n_y - 1], part_send)


def shards(coh_map, positions, counts):
    n_seg, n_lat = lax.axis_size("seg"), lax.axis_size("lat")
    _, bins, width = coh_map.shape
    points = positions.shape[1]
    blocks = counts.shape[0]
    slots = 2 * points // n_lat
    n_y = n_seg // PAIR
    dma = pltpu.SemaphoreType.DMA
    vmem = pl.BlockSpec(memory_space=pltpu.VMEM)
    return pl.pallas_call(
        functools.partial(kernel, n_seg, n_lat),
        out_shape=(
            jax.ShapeDtypeStruct((points, width), jnp.bfloat16),
            jax.ShapeDtypeStruct((blocks, width), jnp.float32),
        ),
        in_specs=[
            pl.BlockSpec(memory_space=pl.ANY),
            vmem,
            pl.BlockSpec(memory_space=pltpu.SMEM),
        ],
        out_specs=(vmem, vmem),
        scratch_shapes=[
            pltpu.VMEM((bins, width), jnp.bfloat16),
            pltpu.VMEM((2, points), jnp.int32),
            pltpu.VMEM((n_lat, 2, points), jnp.int32),
            pltpu.VMEM((2, points), jnp.int32),
            pltpu.VMEM((n_lat, slots + 1, width), jnp.float32),
            pltpu.VMEM((PAIR, n_lat, slots + 1, width), jnp.float32),
            pltpu.VMEM((points, PAIR * n_lat * slots), jnp.bfloat16),
            pltpu.VMEM((n_y, points + 8, width), jnp.float32),
            dma,
            dma,
            dma,
            dma,
            dma((2,)),
            dma((PAIR,)),
            dma,
            dma,
        ],
        compiler_params=pltpu.CompilerParams(collective_id=0, has_side_effects=True),
    )(coh_map, positions, counts)


def solution(mesh):
    in_specs = (P("seg", "lat", None), P("seg", "lat"), P("lat"))
    out_specs = (P("lat", None), P("lat", None))
    return jax.shard_map(shards, mesh=mesh, in_specs=in_specs, out_specs=out_specs, check_vma=False)
```

```python
import functools

import jax
import jax.numpy as jnp
from jax import lax
from jax.experimental import pallas as pl
from jax.experimental.pallas import tpu as pltpu
from jax.sharding import PartitionSpec as P

MESH = pl.DeviceIdType.MESH
PER_BIN = 256
SUB = 4
PAIR = 2
LIVE = 4.0
VALID = 4096.0


def wait_bytes(ref, sem):
    pltpu.make_async_copy(ref, ref, sem).wait()


def kernel(
    n_seg,
    n_lat,
    map_ref,
    pos_ref,
    cnt_ref,
    stat_ref,
    exc_ref,
    table,
    note,
    heard,
    pair_note,
    rows_out,
    rows_in,
    sum_out,
    sum_in,
    pick,
    part,
    table_sem,
    note_send,
    heard_sem,
    pair_sem,
    rows_send,
    rows_sem,
    sum_send,
    sum_sem,
    part_send,
    part_sem,
):
    n_y = n_seg // PAIR
    n_z = n_lat // SUB
    half = n_z // 2
    bins, width = table.shape
    points = pos_ref.shape[1]
    blocks = exc_ref.shape[0]
    block_size = points // blocks
    slots = 2 * points // n_lat
    span = bins * PER_BIN
    f32, bf16, i32 = jnp.float32, jnp.bfloat16, jnp.int32

    seg = lax.axis_index("seg")
    lat = lax.axis_index("lat")
    group, y = lax.div(seg, n_y), lax.rem(seg, n_y)
    other = PAIR - 1 - group
    other_seg = other * n_y + y
    z, q = lax.div(lat, SUB), lax.rem(lat, SUB)

    offsets = [0] + [o for k in range(1, half) for o in (k, n_z - k)] + [half]
    waves = [(0, 1)] + [(2 * k - 1, 2 * k + 1) for k in range(1, half)] + [(n_z - 1, n_z)]
    first_at = [lax.rem(z + o, n_z) * SUB for o in offsets]
    near_q = [lax.rem(q + s, SUB) for s in range(1, SUB)]

    def peers(i):
        if i == 0:
            return [(nq, first_at[0] + nq) for nq in near_q]
        return [(s, first_at[i] + s) for s in range(SUB)]

    y_peers = [group * n_y + lax.rem(y + k, n_y) for k in range(1, n_y)]
    far_first = list(range(n_z - 1, -1, -1))

    load = pltpu.make_async_copy(map_ref.at[0], table, table_sem)
    load.start()

    barrier = pltpu.get_barrier_semaphore()
    for i in far_first:
        for _, d in peers(i):
            pl.semaphore_signal(barrier, inc=1, device_id=(seg, d), device_id_type=MESH)
    pl.semaphore_signal(barrier, inc=1, device_id=(other_seg, lat), device_id_type=MESH)
    for peer in y_peers:
        pl.semaphore_signal(barrier, inc=1, device_id=(peer, lat), device_id_type=MESH)

    lane = lax.broadcasted_iota(i32, (1, points), 1)
    limit = jnp.zeros((1, points), i32)
    for b in range(blocks):
        limit = jnp.where(lane // block_size == b, cnt_ref[b] + b * block_size, limit)
    note[0:1, :] = pos_ref[...]
    note[1:2, :] = jnp.where(lane < limit, 1, 0)

    before_mat = jnp.where(
        lax.broadcasted_iota(i32, (points, points), 0)
        < lax.broadcasted_iota(i32, (points, points), 1),
        1.0,
        0.0,
    ).astype(bf16)
    dest_id = lax.broadcasted_iota(i32, (n_lat, points), 0)
    flat_id = lax.broadcasted_iota(i32, (n_lat * slots, points), 0).astype(f32)

    def chooser(positions):
        dest = lax.div(positions, span)
        at_dest = jnp.where(dest == dest_id, 1.0, 0.0)
        ahead = jnp.dot(at_dest.astype(bf16), before_mat, preferred_element_type=f32)
        slot = jnp.sum(at_dest * ahead, axis=0, keepdims=True)
        flat = dest.astype(f32) * slots + slot
        return jnp.where(flat_id == flat, 1.0, 0.0).T.astype(bf16)

    pick[group] = chooser(pos_ref[...])

    pl.semaphore_wait(barrier, n_lat - 1 + 1 + n_y - 1)

    for i in far_first:
        w = min(offsets[i], n_z - offsets[i])
        back = offsets.index((n_z - offsets[i]) % n_z)
        for _, d in peers(i):
            pltpu.make_async_remote_copy(
                src_ref=note,
                dst_ref=heard.at[back, q],
                send_sem=note_send,
                recv_sem=heard_sem.at[w],
                device_id=(seg, d),
                device_id_type=MESH,
            ).start()
        if i == n_z - 1:
            pltpu.make_async_remote_copy(
                src_ref=note,
                dst_ref=pair_note,
                send_sem=note_send,
                recv_sem=pair_sem,
                device_id=(other_seg, lat),
                device_id_type=MESH,
            ).start()
    pltpu.make_async_copy(note, heard.at[0, q], heard_sem.at[0]).start()

    load.wait()
    bin_id = lax.broadcasted_iota(i32, (1, bins), 1).astype(f32)
    total_sum = jnp.zeros((1, width), f32)
    total_count = jnp.zeros((1, 1), f32)
    for k, (lo, hi) in enumerate(waves):
        wait_bytes(heard.at[lo:hi], heard_sem.at[k])
        n = (hi - lo) * SUB
        pos = heard[lo:hi, :, 0, :].reshape(n, points)
        ok = heard[lo:hi, :, 1, :].reshape(n, points)
        rel = pos - lat * span
        hit = (rel >= 0) & (rel < span)
        before = jnp.dot(
            jnp.where(hit, 1.0, 0.0).astype(bf16), before_mat, preferred_element_type=f32
        )
        key = jnp.where(hit, before, -1.0)
        valid = ok.astype(f32)
        coded = jnp.where(hit, rel.astype(f32) * (1.0 / PER_BIN) + LIVE + valid * VALID, 0.0)
        slot_id = lax.broadcasted_iota(i32, (n, slots, points), 1).astype(f32)
        chosen = jnp.where(key[:, None, :] == slot_id, coded[:, None, :], 0.0)
        code = jnp.sum(chosen, axis=2, keepdims=True).reshape(n * slots, 1)
        is_valid = code >= VALID
        at_bin = code - jnp.where(is_valid, VALID + LIVE, LIVE)
        weights = jnp.maximum(1.0 - jnp.abs(at_bin - bin_id), 0.0).astype(bf16)
        rows = jnp.dot(weights, table[...], preferred_element_type=f32)
        rows_out[lo:hi] = rows.reshape(hi - lo, SUB, slots, width)
        if k == 0:
            wait_bytes(pair_note, pair_sem)

        for i in range(lo, hi):
            targets = [(other_seg, s, first_at[i] + s, 1) for s in range(SUB)]
            targets += [(seg, s, d, 0) for s, d in peers(i)]
            for g, s, d, which in targets:
                pltpu.make_async_remote_copy(
                    src_ref=rows_out.at[i, s],
                    dst_ref=rows_in.at[group, lat],
                    send_sem=rows_send.at[which],
                    recv_sem=rows_sem.at[group],
                    device_id=(g, d),
                    device_id_type=MESH,
                ).start()
            if i == 0:
                pltpu.make_async_copy(
                    rows_out.at[0, q], rows_in.at[group, lat], rows_sem.at[group]
                ).start()
        total_sum += jnp.sum(jnp.where(is_valid, rows, 0.0), axis=0, keepdims=True)
        total_count += jnp.sum(valid, keepdims=True)

    sum_out[...] = jnp.broadcast_to(total_sum, (8, width))
    for i in far_first:
        targets = [(other_seg, s, first_at[i] + s, 1) for s in range(SUB)]
        targets += [(seg, s, d, 0) for s, d in peers(i)]
        for g, s, d, which in targets:
            pltpu.make_async_remote_copy(
                src_ref=sum_out.at[0:1],
                dst_ref=sum_in.at[group, lat],
                send_sem=sum_send.at[which],
                recv_sem=sum_sem,
                device_id=(g, d),
                device_id_type=MESH,
            ).start()
    pltpu.make_async_copy(sum_out.at[0:1], sum_in.at[group, lat], sum_sem).start()

    pick[other] = chooser(pair_note[0:1, :])

    own = jnp.zeros((points, width), f32)
    for g in range(PAIR):
        wait_bytes(rows_in.at[g], rows_sem.at[g])
        got = rows_in[g].reshape(n_lat * slots, width)
        high = got.astype(bf16)
        rest = got - high.astype(f32)
        mid = rest.astype(bf16)
        low = (rest - mid.astype(f32)).astype(bf16)
        choice = pick[g]
        own += (
            jnp.dot(choice, low, preferred_element_type=f32)
            + jnp.dot(choice, mid, preferred_element_type=f32)
            + jnp.dot(choice, high, preferred_element_type=f32)
        )
    part[y, 0:points, :] = own
    wait_bytes(sum_in, sum_sem)
    sums = sum_in[...].reshape(PAIR * n_lat, width)
    part[y, points : points + 8, :] = jnp.broadcast_to(
        jnp.sum(sums, axis=0, keepdims=True), (8, width)
    )

    for peer in y_peers[1:] + y_peers[:1]:
        pltpu.make_async_remote_copy(
            src_ref=part.at[y],
            dst_ref=part.at[y],
            send_sem=part_send,
            recv_sem=part_sem,
            device_id=(peer, lat),
            device_id_type=MESH,
        ).start()
    wait_bytes(part.at[0 : n_y - 1], part_sem)

    all_sum = part[0]
    for k in range(1, n_y):
        all_sum = all_sum + part[k]
    stat = all_sum[0:points] * (1.0 / n_seg)
    stat_ref[...] = stat.astype(bf16)
    global_mean = all_sum[points : points + 1] * (1.0 / n_seg) / total_count
    row_id = lax.broadcasted_iota(i32, (block_size, width), 0)
    for b in range(blocks):
        count = cnt_ref[b]
        block = stat[b * block_size : (b + 1) * block_size]
        block_sum = jnp.sum(jnp.where(row_id < count, block, 0.0), axis=0, keepdims=True)
        exc_ref[b : b + 1, :] = block_sum / count.astype(f32) - global_mean

    wait_bytes(heard, note_send)
    wait_bytes(rows_in.at[0, 0 : n_lat - 1], rows_send.at[0])
    wait_bytes(rows_in.at[0], rows_send.at[1])
    wait_bytes(sum_in.at[0, 0 : n_lat - 1], sum_send.at[0])
    wait_bytes(sum_in.at[0], sum_send.at[1])
    wait_bytes(part.at[0 : n_y - 1], part_send)


def shards(coh_map, positions, counts):
    n_seg, n_lat = lax.axis_size("seg"), lax.axis_size("lat")
    _, bins, width = coh_map.shape
    points = positions.shape[1]
    blocks = counts.shape[0]
    slots = 2 * points // n_lat
    n_y, n_z = n_seg // PAIR, n_lat // SUB
    dma = pltpu.SemaphoreType.DMA
    vmem = pl.BlockSpec(memory_space=pltpu.VMEM)
    return pl.pallas_call(
        functools.partial(kernel, n_seg, n_lat),
        out_shape=(
            jax.ShapeDtypeStruct((points, width), jnp.bfloat16),
            jax.ShapeDtypeStruct((blocks, width), jnp.float32),
        ),
        in_specs=[
            pl.BlockSpec(memory_space=pl.ANY),
            vmem,
            pl.BlockSpec(memory_space=pltpu.SMEM),
        ],
        out_specs=(vmem, vmem),
        scratch_shapes=[
            pltpu.VMEM((bins, width), jnp.bfloat16),
            pltpu.VMEM((2, points), jnp.int32),
            pltpu.VMEM((n_z, SUB, 2, points), jnp.int32),
            pltpu.VMEM((2, points), jnp.int32),
            pltpu.VMEM((n_z, SUB, slots, width), jnp.float32),
            pltpu.VMEM((PAIR, n_lat, slots, width), jnp.float32),
            pltpu.VMEM((8, width), jnp.float32),
            pltpu.VMEM((PAIR, n_lat, 1, width), jnp.float32),
            pltpu.VMEM((PAIR, points, n_lat * slots), jnp.bfloat16),
            pltpu.VMEM((n_y, points + 8, width), jnp.float32),
            dma,
            dma,
            dma((n_z // 2 + 1,)),
            dma,
            dma((2,)),
            dma((PAIR,)),
            dma((2,)),
            dma,
            dma,
            dma,
        ],
        compiler_params=pltpu.CompilerParams(collective_id=0, has_side_effects=True),
    )(coh_map, positions, counts)


def solution(mesh):
    in_specs = (P("seg", "lat", None), P("seg", "lat"), P("lat"))
    out_specs = (P("lat", None), P("lat", None))
    return jax.shard_map(shards, mesh=mesh, in_specs=in_specs, out_specs=out_specs, check_vma=False)
```

```python
import functools

import jax
import jax.numpy as jnp
from jax import lax
from jax.experimental import pallas as pl
from jax.experimental.pallas import tpu as pltpu
from jax.sharding import PartitionSpec as P

MESH = pl.DeviceIdType.MESH
PER_BIN = 256
SUB = 4
PAIR = 2
LIVE = 4.0
VALID = 4096.0


def wait_bytes(ref, sem):
    pltpu.make_async_copy(ref, ref, sem).wait()


def kernel(
    n_seg,
    n_lat,
    map_ref,
    pos_hbm,
    cnt_hbm,
    stat_ref,
    exc_ref,
    table,
    cnt_ref,
    note,
    heard,
    pair_note,
    rows_out,
    rows_in,
    sum_out,
    near_in,
    far_in,
    pick,
    part,
    pos_sem,
    cnt_sem,
    table_sem,
    note_send,
    heard_sem,
    pair_sem,
    rows_send,
    rows_sem,
    sum_send,
    near_sem,
    far_sem,
    part_send,
    part_sem,
):
    n_y = n_seg // PAIR
    n_z = n_lat // SUB
    half = n_z // 2
    bins, width = table.shape
    points = pos_hbm.shape[1]
    blocks = exc_ref.shape[0]
    block_size = points // blocks
    slots = 2 * points // n_lat
    span = bins * PER_BIN
    f32, bf16, i32 = jnp.float32, jnp.bfloat16, jnp.int32

    seg = lax.axis_index("seg")
    lat = lax.axis_index("lat")
    group, y = lax.div(seg, n_y), lax.rem(seg, n_y)
    other = PAIR - 1 - group
    other_seg = other * n_y + y
    z, q = lax.div(lat, SUB), lax.rem(lat, SUB)

    offsets = [0] + [o for k in range(1, half) for o in (k, n_z - k)] + [half]
    waves = [(0, 1)] + [(2 * k - 1, 2 * k + 1) for k in range(1, half)] + [(n_z - 1, n_z)]
    first_at = [lax.rem(z + o, n_z) * SUB for o in offsets]
    near_q = [lax.rem(q + s, SUB) for s in range(1, SUB)]

    def peers(i):
        if i == 0:
            return [(nq, first_at[0] + nq) for nq in near_q]
        return [(s, first_at[i] + s) for s in range(SUB)]

    y_peers = [group * n_y + lax.rem(y + k, n_y) for k in range(1, n_y)]
    far_first = list(range(n_z - 1, -1, -1))

    load_pos = pltpu.make_async_copy(pos_hbm, note.at[0:1], pos_sem)
    load_cnt = pltpu.make_async_copy(cnt_hbm, cnt_ref, cnt_sem)
    load = pltpu.make_async_copy(map_ref.at[0], table, table_sem)
    load_pos.start()
    load_cnt.start()

    barrier = pltpu.get_barrier_semaphore()
    for i in far_first:
        for _, d in peers(i):
            pl.semaphore_signal(barrier, inc=1, device_id=(seg, d), device_id_type=MESH)
    pl.semaphore_signal(barrier, inc=1, device_id=(other_seg, lat), device_id_type=MESH)
    for peer in y_peers:
        pl.semaphore_signal(barrier, inc=1, device_id=(peer, lat), device_id_type=MESH)

    load.start()

    lane = lax.broadcasted_iota(i32, (1, points), 1)
    limit = jnp.zeros((1, points), i32)
    load_cnt.wait()
    for b in range(blocks):
        limit = jnp.where(lane // block_size == b, cnt_ref[b] + b * block_size, limit)
    note[1:2, :] = jnp.where(lane < limit, 1, 0)

    before_mat = jnp.where(
        lax.broadcasted_iota(i32, (points, points), 0)
        < lax.broadcasted_iota(i32, (points, points), 1),
        1.0,
        0.0,
    ).astype(bf16)
    dest_id = lax.broadcasted_iota(i32, (n_lat, points), 0)
    flat_id = lax.broadcasted_iota(i32, (n_lat * slots, points), 0).astype(f32)

    def chooser(positions):
        dest = lax.div(positions, span)
        at_dest = jnp.where(dest == dest_id, 1.0, 0.0)
        ahead = jnp.dot(at_dest.astype(bf16), before_mat, preferred_element_type=f32)
        slot = jnp.sum(at_dest * ahead, axis=0, keepdims=True)
        flat = dest.astype(f32) * slots + slot
        return jnp.where(flat_id == flat, 1.0, 0.0).T.astype(bf16)

    load_pos.wait()
    pick[group] = chooser(note[0:1, :])

    pl.semaphore_wait(barrier, n_lat - 1 + 1 + n_y - 1)

    for i in far_first:
        w = min(offsets[i], n_z - offsets[i])
        back = offsets.index((n_z - offsets[i]) % n_z)
        for _, d in peers(i):
            pltpu.make_async_remote_copy(
                src_ref=note,
                dst_ref=heard.at[back, q],
                send_sem=note_send,
                recv_sem=heard_sem.at[w],
                device_id=(seg, d),
                device_id_type=MESH,
            ).start()
        if i == n_z - 1:
            pltpu.make_async_remote_copy(
                src_ref=note,
                dst_ref=pair_note,
                send_sem=note_send,
                recv_sem=pair_sem,
                device_id=(other_seg, lat),
                device_id_type=MESH,
            ).start()
    pltpu.make_async_copy(note, heard.at[0, q], heard_sem.at[0]).start()

    load.wait()
    bin_id = lax.broadcasted_iota(i32, (1, bins), 1).astype(f32)
    total_sum = jnp.zeros((1, width), f32)
    total_count = jnp.zeros((1, 1), f32)
    for k, (lo, hi) in enumerate(waves):
        wait_bytes(heard.at[lo:hi], heard_sem.at[k])
        n = (hi - lo) * SUB
        pos = heard[lo:hi, :, 0, :].reshape(n, points)
        ok = heard[lo:hi, :, 1, :].reshape(n, points)
        rel = pos - lat * span
        hit = (rel >= 0) & (rel < span)
        before = jnp.dot(
            jnp.where(hit, 1.0, 0.0).astype(bf16), before_mat, preferred_element_type=f32
        )
        key = jnp.where(hit, before, -1.0)
        valid = ok.astype(f32)
        coded = jnp.where(hit, rel.astype(f32) * (1.0 / PER_BIN) + LIVE + valid * VALID, 0.0)
        slot_id = lax.broadcasted_iota(i32, (n, slots, points), 1).astype(f32)
        chosen = jnp.where(key[:, None, :] == slot_id, coded[:, None, :], 0.0)
        code = jnp.sum(chosen, axis=2, keepdims=True).reshape(n * slots, 1)
        is_valid = code >= VALID
        at_bin = code - jnp.where(is_valid, VALID + LIVE, LIVE)
        weights = jnp.maximum(1.0 - jnp.abs(at_bin - bin_id), 0.0).astype(bf16)
        rows = jnp.dot(weights, table[...], preferred_element_type=f32)
        rows_out[lo:hi] = rows.reshape(hi - lo, SUB, slots, width)
        if k == 0:
            wait_bytes(pair_note, pair_sem)

        for i in range(lo, hi):
            targets = [(other_seg, s, first_at[i] + s, 1) for s in range(SUB)]
            targets += [(seg, s, d, 0) for s, d in peers(i)]
            for g, s, d, which in targets:
                pltpu.make_async_remote_copy(
                    src_ref=rows_out.at[i, s],
                    dst_ref=rows_in.at[group, lat],
                    send_sem=rows_send.at[which],
                    recv_sem=rows_sem.at[group],
                    device_id=(g, d),
                    device_id_type=MESH,
                ).start()
            if i == 0:
                pltpu.make_async_copy(
                    rows_out.at[0, q], rows_in.at[group, lat], rows_sem.at[group]
                ).start()
        total_sum += jnp.sum(jnp.where(is_valid, rows, 0.0), axis=0, keepdims=True)
        total_count += jnp.sum(valid, keepdims=True)

    sum_out[0] = total_sum
    near_in[group * SUB + q] = total_sum
    for g, d in [(other_seg, first_at[0] + s) for s in range(SUB)] + [
        (seg, d) for _, d in peers(0)
    ]:
        pltpu.make_async_remote_copy(
            src_ref=sum_out.at[0],
            dst_ref=near_in.at[group * SUB + q],
            send_sem=sum_send.at[0],
            recv_sem=near_sem,
            device_id=(g, d),
            device_id_type=MESH,
        ).start()

    pick[other] = chooser(pair_note[0:1, :])

    wait_bytes(near_in.at[0 : PAIR * SUB - 1], near_sem)
    near_sum = jnp.sum(near_in[...], axis=0)
    sum_out[1] = near_sum
    far_in[z] = near_sum
    for i in far_first[:-1]:
        pltpu.make_async_remote_copy(
            src_ref=sum_out.at[1],
            dst_ref=far_in.at[z],
            send_sem=sum_send.at[1],
            recv_sem=far_sem,
            device_id=(seg, first_at[i] + q),
            device_id_type=MESH,
        ).start()

    own = jnp.zeros((points, width), f32)
    for g in range(PAIR):
        wait_bytes(rows_in.at[g], rows_sem.at[g])
        got = rows_in[g].reshape(n_lat * slots, width)
        high = got.astype(bf16)
        rest = got - high.astype(f32)
        mid = rest.astype(bf16)
        low = (rest - mid.astype(f32)).astype(bf16)
        choice = pick[g]
        own += (
            jnp.dot(choice, low, preferred_element_type=f32)
            + jnp.dot(choice, mid, preferred_element_type=f32)
            + jnp.dot(choice, high, preferred_element_type=f32)
        )
    part[y, 0:points, :] = own
    wait_bytes(far_in.at[0 : n_z - 1], far_sem)
    part[y, points : points + 8, :] = jnp.broadcast_to(jnp.sum(far_in[...], axis=0), (8, width))

    for peer in y_peers[1:] + y_peers[:1]:
        pltpu.make_async_remote_copy(
            src_ref=part.at[y],
            dst_ref=part.at[y],
            send_sem=part_send,
            recv_sem=part_sem,
            device_id=(peer, lat),
            device_id_type=MESH,
        ).start()
    wait_bytes(part.at[0 : n_y - 1], part_sem)

    all_sum = part[0]
    for k in range(1, n_y):
        all_sum = all_sum + part[k]
    stat = all_sum[0:points] * (1.0 / n_seg)
    stat_ref[...] = stat.astype(bf16)
    global_mean = all_sum[points : points + 1] * (1.0 / n_seg) / total_count
    row_id = lax.broadcasted_iota(i32, (block_size, width), 0)
    for b in range(blocks):
        count = cnt_ref[b]
        block = stat[b * block_size : (b + 1) * block_size]
        block_sum = jnp.sum(jnp.where(row_id < count, block, 0.0), axis=0, keepdims=True)
        exc_ref[b : b + 1, :] = block_sum / count.astype(f32) - global_mean

    wait_bytes(heard, note_send)
    wait_bytes(rows_in.at[0, 0 : n_lat - 1], rows_send.at[0])
    wait_bytes(rows_in.at[0], rows_send.at[1])
    wait_bytes(near_in.at[0 : PAIR * SUB - 1], sum_send.at[0])
    wait_bytes(far_in.at[0 : n_z - 1], sum_send.at[1])
    wait_bytes(part.at[0 : n_y - 1], part_send)


def put_out(stat_ref, exc_ref, stat_out, exc_out, stat_sem, exc_sem):
    stat = pltpu.make_async_copy(stat_ref, stat_out, stat_sem)
    exc = pltpu.make_async_copy(exc_ref, exc_out, exc_sem)
    stat.start()
    exc.start()
    stat.wait()
    exc.wait()


def shards(coh_map, positions, counts):
    n_seg, n_lat = lax.axis_size("seg"), lax.axis_size("lat")
    _, bins, width = coh_map.shape
    points = positions.shape[1]
    blocks = counts.shape[0]
    slots = 2 * points // n_lat
    n_y, n_z = n_seg // PAIR, n_lat // SUB
    dma = pltpu.SemaphoreType.DMA
    vmem = pl.BlockSpec(memory_space=pltpu.VMEM)
    anywhere = pl.BlockSpec(memory_space=pl.ANY)
    stat, excess = pl.pallas_call(
        functools.partial(kernel, n_seg, n_lat),
        out_shape=(
            pltpu.VMEM((points, width), jnp.bfloat16),
            pltpu.VMEM((blocks, width), jnp.float32),
        ),
        in_specs=[
            anywhere,
            anywhere,
            anywhere,
        ],
        out_specs=(vmem, vmem),
        scratch_shapes=[
            pltpu.VMEM((bins, width), jnp.bfloat16),
            pltpu.SMEM((blocks,), jnp.int32),
            pltpu.VMEM((2, points), jnp.int32),
            pltpu.VMEM((n_z, SUB, 2, points), jnp.int32),
            pltpu.VMEM((2, points), jnp.int32),
            pltpu.VMEM((n_z, SUB, slots, width), jnp.float32),
            pltpu.VMEM((PAIR, n_lat, slots, width), jnp.float32),
            pltpu.VMEM((2, 1, width), jnp.float32),
            pltpu.VMEM((PAIR * SUB, 1, width), jnp.float32),
            pltpu.VMEM((n_z, 1, width), jnp.float32),
            pltpu.VMEM((PAIR, points, n_lat * slots), jnp.bfloat16),
            pltpu.VMEM((n_y, points + 8, width), jnp.float32),
            dma,
            dma,
            dma,
            dma,
            dma((n_z // 2 + 1,)),
            dma,
            dma((2,)),
            dma((PAIR,)),
            dma((2,)),
            dma,
            dma,
            dma,
            dma,
        ],
        compiler_params=pltpu.CompilerParams(collective_id=0, has_side_effects=True),
    )(coh_map, positions, counts)
    in_vmem = functools.partial(pltpu.with_memory_space_constraint, memory_space=pltpu.VMEM)
    return pl.pallas_call(
        put_out,
        out_shape=(
            jax.ShapeDtypeStruct((points, width), jnp.bfloat16),
            jax.ShapeDtypeStruct((blocks, width), jnp.float32),
        ),
        in_specs=[vmem, vmem],
        out_specs=(anywhere, anywhere),
        scratch_shapes=[dma, dma],
    )(in_vmem(stat), in_vmem(excess))


def solution(mesh):
    in_specs = (P("seg", "lat", None), P("seg", "lat"), P("lat"))
    out_specs = (P("lat", None), P("lat", None))
    return jax.shard_map(shards, mesh=mesh, in_specs=in_specs, out_specs=out_specs, check_vma=False)
```

```python
import functools

import jax
import jax.numpy as jnp
from jax import lax
from jax.experimental import pallas as pl
from jax.experimental.pallas import tpu as pltpu
from jax.sharding import PartitionSpec as P

MESH = pl.DeviceIdType.MESH
PER_BIN = 256
SUB = 4
PAIR = 2
LIVE = 4.0
VALID = 4096.0


def wait_bytes(ref, sem):
    pltpu.make_async_copy(ref, ref, sem).wait()


def kernel(
    n_seg,
    n_lat,
    map_ref,
    pos_hbm,
    cnt_hbm,
    stat_ref,
    exc_ref,
    table,
    cnt_ref,
    note,
    heard,
    pair_note,
    rows_out,
    rows_in,
    sum_out,
    near_in,
    far_in,
    pick,
    part,
    pos_sem,
    cnt_sem,
    table_sem,
    note_send,
    heard_sem,
    pair_sem,
    rows_send,
    rows_sem,
    sum_send,
    near_sem,
    far_sem,
    part_send,
    part_sem,
):
    n_y = n_seg // PAIR
    n_z = n_lat // SUB
    half = n_z // 2
    bins, width = table.shape
    points = pos_hbm.shape[1]
    blocks = exc_ref.shape[0]
    block_size = points // blocks
    slots = 2 * points // n_lat
    span = bins * PER_BIN
    f32, bf16, i32 = jnp.float32, jnp.bfloat16, jnp.int32

    seg = lax.axis_index("seg")
    lat = lax.axis_index("lat")
    group, y = lax.div(seg, n_y), lax.rem(seg, n_y)
    other = PAIR - 1 - group
    other_seg = other * n_y + y
    z, q = lax.div(lat, SUB), lax.rem(lat, SUB)

    offsets = [0] + [o for k in range(1, half) for o in (k, n_z - k)] + [half]
    waves = [(0, 1)] + [(2 * k - 1, 2 * k + 1) for k in range(1, half)] + [(n_z - 1, n_z)]
    first_at = [lax.rem(z + o, n_z) * SUB for o in offsets]
    near_q = [lax.rem(q + s, SUB) for s in range(1, SUB)]

    def peers(i):
        if i == 0:
            return [(nq, first_at[0] + nq) for nq in near_q]
        return [(s, first_at[i] + s) for s in range(SUB)]

    y_peers = [group * n_y + lax.rem(y + k, n_y) for k in range(1, n_y)]
    far_first = list(range(n_z - 1, -1, -1))

    load_pos = pltpu.make_async_copy(pos_hbm, note.at[0:1], pos_sem)
    load_cnt = pltpu.make_async_copy(cnt_hbm, cnt_ref, cnt_sem)
    load = pltpu.make_async_copy(map_ref.at[0], table, table_sem)
    load_pos.start()
    load_cnt.start()

    barrier = pltpu.get_barrier_semaphore()
    for i in far_first:
        for _, d in peers(i):
            pl.semaphore_signal(barrier, inc=1, device_id=(seg, d), device_id_type=MESH)
    pl.semaphore_signal(barrier, inc=1, device_id=(other_seg, lat), device_id_type=MESH)
    for peer in y_peers:
        pl.semaphore_signal(barrier, inc=1, device_id=(peer, lat), device_id_type=MESH)

    load.start()

    lane = lax.broadcasted_iota(i32, (1, points), 1)
    limit = jnp.zeros((1, points), i32)
    load_cnt.wait()
    for b in range(blocks):
        limit = jnp.where(lane // block_size == b, cnt_ref[b] + b * block_size, limit)
    note[1:2, :] = jnp.where(lane < limit, 1, 0)

    before_mat = jnp.where(
        lax.broadcasted_iota(i32, (points, points), 0)
        < lax.broadcasted_iota(i32, (points, points), 1),
        1.0,
        0.0,
    ).astype(bf16)
    dest_id = lax.broadcasted_iota(i32, (n_lat, points), 0)
    flat_id = lax.broadcasted_iota(i32, (n_lat * slots, points), 0).astype(f32)

    def chooser(positions):
        dest = lax.div(positions, span)
        at_dest = jnp.where(dest == dest_id, 1.0, 0.0)
        ahead = jnp.dot(at_dest.astype(bf16), before_mat, preferred_element_type=f32)
        slot = jnp.sum(at_dest * ahead, axis=0, keepdims=True)
        flat = dest.astype(f32) * slots + slot
        return jnp.where(flat_id == flat, 1.0, 0.0).T.astype(bf16)

    load_pos.wait()
    pick[group] = chooser(note[0:1, :])

    pl.semaphore_wait(barrier, n_lat - 1 + 1 + n_y - 1)

    for i in far_first:
        w = min(offsets[i], n_z - offsets[i])
        back = offsets.index((n_z - offsets[i]) % n_z)
        for _, d in peers(i):
            pltpu.make_async_remote_copy(
                src_ref=note,
                dst_ref=heard.at[back, q],
                send_sem=note_send,
                recv_sem=heard_sem.at[w],
                device_id=(seg, d),
                device_id_type=MESH,
            ).start()
        if i == n_z - 1:
            pltpu.make_async_remote_copy(
                src_ref=note,
                dst_ref=pair_note,
                send_sem=note_send,
                recv_sem=pair_sem,
                device_id=(other_seg, lat),
                device_id_type=MESH,
            ).start()
    pltpu.make_async_copy(note, heard.at[0, q], heard_sem.at[0]).start()

    def give(k, to_seg, which):
        for i in range(*waves[k]):
            slice_ids = range(SUB) if which else [s for s, _ in peers(i)]
            for s in slice_ids:
                pltpu.make_async_remote_copy(
                    src_ref=rows_out.at[i, s],
                    dst_ref=rows_in.at[group, lat],
                    send_sem=rows_send.at[which],
                    recv_sem=rows_sem.at[group],
                    device_id=(to_seg, first_at[i] + s),
                    device_id_type=MESH,
                ).start()

    held = half // 2
    load.wait()
    bin_id = lax.broadcasted_iota(i32, (1, bins), 1).astype(f32)
    total_sum = jnp.zeros((1, width), f32)
    total_count = jnp.zeros((1, 1), f32)
    for k, (lo, hi) in enumerate(waves):
        wait_bytes(heard.at[lo:hi], heard_sem.at[k])
        n = (hi - lo) * SUB
        pos = heard[lo:hi, :, 0, :].reshape(n, points)
        ok = heard[lo:hi, :, 1, :].reshape(n, points)
        rel = pos - lat * span
        hit = (rel >= 0) & (rel < span)
        before = jnp.dot(
            jnp.where(hit, 1.0, 0.0).astype(bf16), before_mat, preferred_element_type=f32
        )
        key = jnp.where(hit, before, -1.0)
        valid = ok.astype(f32)
        coded = jnp.where(hit, rel.astype(f32) * (1.0 / PER_BIN) + LIVE + valid * VALID, 0.0)
        slot_id = lax.broadcasted_iota(i32, (n, slots, points), 1).astype(f32)
        chosen = jnp.where(key[:, None, :] == slot_id, coded[:, None, :], 0.0)
        code = jnp.sum(chosen, axis=2, keepdims=True).reshape(n * slots, 1)
        is_valid = code >= VALID
        at_bin = code - jnp.where(is_valid, VALID + LIVE, LIVE)
        weights = jnp.maximum(1.0 - jnp.abs(at_bin - bin_id), 0.0).astype(bf16)
        rows = jnp.dot(weights, table[...], preferred_element_type=f32)
        rows_out[lo:hi] = rows.reshape(hi - lo, SUB, slots, width)
        if k == 0:
            wait_bytes(pair_note, pair_sem)
            pltpu.make_async_copy(
                rows_out.at[0, q], rows_in.at[group, lat], rows_sem.at[group]
            ).start()
        if k != held:
            give(k, other_seg, 1)
        give(k, seg, 0)
        if k == len(waves) - 1:
            give(held, other_seg, 1)
        total_sum += jnp.sum(jnp.where(is_valid, rows, 0.0), axis=0, keepdims=True)
        total_count += jnp.sum(valid, keepdims=True)

    sum_out[0] = total_sum
    near_in[group * SUB + q] = total_sum
    for g, d in [(other_seg, first_at[0] + s) for s in range(SUB)] + [
        (seg, d) for _, d in peers(0)
    ]:
        pltpu.make_async_remote_copy(
            src_ref=sum_out.at[0],
            dst_ref=near_in.at[group * SUB + q],
            send_sem=sum_send.at[0],
            recv_sem=near_sem,
            device_id=(g, d),
            device_id_type=MESH,
        ).start()

    pick[other] = chooser(pair_note[0:1, :])

    wait_bytes(near_in.at[0 : PAIR * SUB - 1], near_sem)
    near_sum = jnp.sum(near_in[...], axis=0)
    sum_out[1] = near_sum
    far_in[z] = near_sum
    for i in far_first[:-1]:
        pltpu.make_async_remote_copy(
            src_ref=sum_out.at[1],
            dst_ref=far_in.at[z],
            send_sem=sum_send.at[1],
            recv_sem=far_sem,
            device_id=(seg, first_at[i] + q),
            device_id_type=MESH,
        ).start()

    own = jnp.zeros((points, width), f32)
    for g in range(PAIR):
        wait_bytes(rows_in.at[g], rows_sem.at[g])
        got = rows_in[g].reshape(n_lat * slots, width)
        high = got.astype(bf16)
        rest = got - high.astype(f32)
        mid = rest.astype(bf16)
        low = (rest - mid.astype(f32)).astype(bf16)
        choice = pick[g]
        own += (
            jnp.dot(choice, low, preferred_element_type=f32)
            + jnp.dot(choice, mid, preferred_element_type=f32)
            + jnp.dot(choice, high, preferred_element_type=f32)
        )
    part[y, 0:points, :] = own
    wait_bytes(far_in.at[0 : n_z - 1], far_sem)
    part[y, points : points + 8, :] = jnp.broadcast_to(jnp.sum(far_in[...], axis=0), (8, width))

    for peer in y_peers[1:] + y_peers[:1]:
        pltpu.make_async_remote_copy(
            src_ref=part.at[y],
            dst_ref=part.at[y],
            send_sem=part_send,
            recv_sem=part_sem,
            device_id=(peer, lat),
            device_id_type=MESH,
        ).start()
    wait_bytes(part.at[0 : n_y - 1], part_sem)

    all_sum = part[0]
    for k in range(1, n_y):
        all_sum = all_sum + part[k]
    stat = all_sum[0:points] * (1.0 / n_seg)
    stat_ref[...] = stat.astype(bf16)
    global_mean = all_sum[points : points + 1] * (1.0 / n_seg) / total_count
    row_id = lax.broadcasted_iota(i32, (block_size, width), 0)
    for b in range(blocks):
        count = cnt_ref[b]
        block = stat[b * block_size : (b + 1) * block_size]
        block_sum = jnp.sum(jnp.where(row_id < count, block, 0.0), axis=0, keepdims=True)
        exc_ref[b : b + 1, :] = block_sum / count.astype(f32) - global_mean

    wait_bytes(heard, note_send)
    wait_bytes(rows_in.at[0, 0 : n_lat - 1], rows_send.at[0])
    wait_bytes(rows_in.at[0], rows_send.at[1])
    wait_bytes(near_in.at[0 : PAIR * SUB - 1], sum_send.at[0])
    wait_bytes(far_in.at[0 : n_z - 1], sum_send.at[1])
    wait_bytes(part.at[0 : n_y - 1], part_send)


def put_out(stat_ref, exc_ref, stat_out, exc_out, stat_sem, exc_sem):
    stat = pltpu.make_async_copy(stat_ref, stat_out, stat_sem)
    exc = pltpu.make_async_copy(exc_ref, exc_out, exc_sem)
    stat.start()
    exc.start()
    stat.wait()
    exc.wait()


def shards(coh_map, positions, counts):
    n_seg, n_lat = lax.axis_size("seg"), lax.axis_size("lat")
    _, bins, width = coh_map.shape
    points = positions.shape[1]
    blocks = counts.shape[0]
    slots = 2 * points // n_lat
    n_y, n_z = n_seg // PAIR, n_lat // SUB
    dma = pltpu.SemaphoreType.DMA
    vmem = pl.BlockSpec(memory_space=pltpu.VMEM)
    anywhere = pl.BlockSpec(memory_space=pl.ANY)
    stat, excess = pl.pallas_call(
        functools.partial(kernel, n_seg, n_lat),
        out_shape=(
            pltpu.VMEM((points, width), jnp.bfloat16),
            pltpu.VMEM((blocks, width), jnp.float32),
        ),
        in_specs=[
            anywhere,
            anywhere,
            anywhere,
        ],
        out_specs=(vmem, vmem),
        scratch_shapes=[
            pltpu.VMEM((bins, width), jnp.bfloat16),
            pltpu.SMEM((blocks,), jnp.int32),
            pltpu.VMEM((2, points), jnp.int32),
            pltpu.VMEM((n_z, SUB, 2, points), jnp.int32),
            pltpu.VMEM((2, points), jnp.int32),
            pltpu.VMEM((n_z, SUB, slots, width), jnp.float32),
            pltpu.VMEM((PAIR, n_lat, slots, width), jnp.float32),
            pltpu.VMEM((2, 1, width), jnp.float32),
            pltpu.VMEM((PAIR * SUB, 1, width), jnp.float32),
            pltpu.VMEM((n_z, 1, width), jnp.float32),
            pltpu.VMEM((PAIR, points, n_lat * slots), jnp.bfloat16),
            pltpu.VMEM((n_y, points + 8, width), jnp.float32),
            dma,
            dma,
            dma,
            dma,
            dma((n_z // 2 + 1,)),
            dma,
            dma((2,)),
            dma((PAIR,)),
            dma((2,)),
            dma,
            dma,
            dma,
            dma,
        ],
        compiler_params=pltpu.CompilerParams(collective_id=0, has_side_effects=True),
    )(coh_map, positions, counts)
    in_vmem = functools.partial(pltpu.with_memory_space_constraint, memory_space=pltpu.VMEM)
    return pl.pallas_call(
        put_out,
        out_shape=(
            jax.ShapeDtypeStruct((points, width), jnp.bfloat16),
            jax.ShapeDtypeStruct((blocks, width), jnp.float32),
        ),
        in_specs=[vmem, vmem],
        out_specs=(anywhere, anywhere),
        scratch_shapes=[dma, dma],
    )(in_vmem(stat), in_vmem(excess))


def solution(mesh):
    in_specs = (P("seg", "lat", None), P("seg", "lat"), P("lat"))
    out_specs = (P("lat", None), P("lat", None))
    return jax.shard_map(shards, mesh=mesh, in_specs=in_specs, out_specs=out_specs, check_vma=False)
```

```python
import functools

import jax
import jax.numpy as jnp
from jax import lax
from jax.experimental import pallas as pl
from jax.experimental.pallas import tpu as pltpu
from jax.sharding import PartitionSpec as P

MESH = pl.DeviceIdType.MESH
PER_BIN = 256
SUB = 4
PAIR = 2
LIVE = 4.0
VALID = 4096.0


def wait_bytes(ref, sem):
    pltpu.make_async_copy(ref, ref, sem).wait()


def kernel(
    n_seg,
    n_lat,
    map_ref,
    pos_hbm,
    cnt_hbm,
    stat_ref,
    exc_ref,
    table,
    cnt_ref,
    note,
    heard,
    pair_note,
    rows_out,
    rows_in,
    sum_out,
    near_in,
    far_in,
    pick,
    part,
    pos_sem,
    cnt_sem,
    table_sem,
    note_send,
    heard_sem,
    pair_sem,
    rows_send,
    rows_sem,
    sum_send,
    near_sem,
    far_sem,
    part_send,
    part_sem,
):
    n_y = n_seg // PAIR
    n_z = n_lat // SUB
    half = n_z // 2
    bins, width = table.shape
    points = pos_hbm.shape[1]
    blocks = exc_ref.shape[0]
    block_size = points // blocks
    slots = 2 * points // n_lat
    span = bins * PER_BIN
    f32, bf16, i32 = jnp.float32, jnp.bfloat16, jnp.int32

    seg = lax.axis_index("seg")
    lat = lax.axis_index("lat")
    group, y = lax.div(seg, n_y), lax.rem(seg, n_y)
    other = PAIR - 1 - group
    other_seg = other * n_y + y
    z, q = lax.div(lat, SUB), lax.rem(lat, SUB)

    offsets = [0] + [o for k in range(1, half) for o in (k, n_z - k)] + [half]
    waves = [(0, 1)] + [(2 * k - 1, 2 * k + 1) for k in range(1, half)] + [(n_z - 1, n_z)]
    first_at = [lax.rem(z + o, n_z) * SUB for o in offsets]
    near_q = [lax.rem(q + s, SUB) for s in range(1, SUB)]

    def peers(i):
        if i == 0:
            return [(nq, first_at[0] + nq) for nq in near_q]
        return [(s, first_at[i] + s) for s in range(SUB)]

    y_peers = [group * n_y + lax.rem(y + k, n_y) for k in range(1, n_y)]
    far_first = list(range(n_z - 1, -1, -1))

    load_pos = pltpu.make_async_copy(pos_hbm, note.at[0:1], pos_sem)
    load_cnt = pltpu.make_async_copy(cnt_hbm, cnt_ref, cnt_sem)
    load = pltpu.make_async_copy(map_ref.at[0], table, table_sem)
    load_pos.start()
    load_cnt.start()

    barrier = pltpu.get_barrier_semaphore()
    for i in far_first:
        for _, d in peers(i):
            pl.semaphore_signal(barrier, inc=1, device_id=(seg, d), device_id_type=MESH)
    pl.semaphore_signal(barrier, inc=1, device_id=(other_seg, lat), device_id_type=MESH)
    for peer in y_peers:
        pl.semaphore_signal(barrier, inc=1, device_id=(peer, lat), device_id_type=MESH)

    load.start()

    lane = lax.broadcasted_iota(i32, (1, points), 1)
    limit = jnp.zeros((1, points), i32)
    load_cnt.wait()
    for b in range(blocks):
        limit = jnp.where(lane // block_size == b, cnt_ref[b] + b * block_size, limit)
    note[1:2, :] = jnp.where(lane < limit, 1, 0)

    before_mat = jnp.where(
        lax.broadcasted_iota(i32, (points, points), 0)
        < lax.broadcasted_iota(i32, (points, points), 1),
        1.0,
        0.0,
    ).astype(bf16)
    hs = slots // 2
    dest_id = lax.broadcasted_iota(i32, (n_lat, points), 0)
    flat_id = lax.broadcasted_iota(i32, (n_lat * hs, points), 0).astype(f32)

    def choose(g, positions):
        dest = lax.div(positions, span)
        at_dest = jnp.where(dest == dest_id, 1.0, 0.0)
        ahead = jnp.dot(at_dest.astype(bf16), before_mat, preferred_element_type=f32)
        slot = jnp.sum(at_dest * ahead, axis=0, keepdims=True)
        base = dest.astype(f32) * hs + slot
        flat_low = jnp.where(slot < hs, base, -1.0)
        flat_high = jnp.where(slot < hs, -1.0, base - hs)
        pick[g, 0:points] = jnp.where(flat_id == flat_low, 1.0, 0.0).T.astype(bf16)
        pick[g, points : 2 * points] = jnp.where(flat_id == flat_high, 1.0, 0.0).T.astype(bf16)

    load_pos.wait()
    choose(group, note[0:1, :])

    pl.semaphore_wait(barrier, n_lat - 1 + 1 + n_y - 1)

    for i in far_first:
        w = min(offsets[i], n_z - offsets[i])
        back = offsets.index((n_z - offsets[i]) % n_z)
        for _, d in peers(i):
            pltpu.make_async_remote_copy(
                src_ref=note,
                dst_ref=heard.at[back, q],
                send_sem=note_send,
                recv_sem=heard_sem.at[w],
                device_id=(seg, d),
                device_id_type=MESH,
            ).start()
        if i == n_z - 1:
            pltpu.make_async_remote_copy(
                src_ref=note,
                dst_ref=pair_note,
                send_sem=note_send,
                recv_sem=pair_sem,
                device_id=(other_seg, lat),
                device_id_type=MESH,
            ).start()
    pltpu.make_async_copy(note, heard.at[0, q], heard_sem.at[0]).start()

    def give(k, h):
        for i in range(*waves[k]):
            targets = [(other_seg, s, first_at[i] + s, 1) for s in range(SUB)]
            targets += [(seg, s, d, 0) for s, d in peers(i)]
            for to_seg, s, d, which in targets:
                pltpu.make_async_remote_copy(
                    src_ref=rows_out.at[h, i, s],
                    dst_ref=rows_in.at[h, group, lat],
                    send_sem=rows_send.at[h, which],
                    recv_sem=rows_sem.at[h, group],
                    device_id=(to_seg, d),
                    device_id_type=MESH,
                ).start()
            if i == 0:
                pltpu.make_async_copy(
                    rows_out.at[h, 0, q], rows_in.at[h, group, lat], rows_sem.at[h, group]
                ).start()

    order = [[(k, 0), (k, 1)] for k in range(len(waves))]
    order[2] = [(2, 0)]
    order[3] = [(3, 0)]
    order[4] = [(4, 0), (3, 1), (4, 1), (2, 1)]
    tile = (1, slots, width)
    upper = lax.broadcasted_iota(i32, tile, 1) >= hs
    right = lax.broadcasted_iota(i32, tile, 2) >= width // 2
    stays = upper == right
    on_left = lax.broadcasted_iota(i32, (1, width), 1) < width // 2

    load.wait()
    bin_id = lax.broadcasted_iota(i32, (1, bins), 1).astype(f32)
    total_sum = jnp.zeros((1, width), f32)
    total_count = jnp.zeros((1, 1), f32)
    for k, (lo, hi) in enumerate(waves):
        wait_bytes(heard.at[lo:hi], heard_sem.at[k])
        n = (hi - lo) * SUB
        pos = heard[lo:hi, :, 0, :].reshape(n, points)
        ok = heard[lo:hi, :, 1, :].reshape(n, points)
        rel = pos - lat * span
        hit = (rel >= 0) & (rel < span)
        before = jnp.dot(
            jnp.where(hit, 1.0, 0.0).astype(bf16), before_mat, preferred_element_type=f32
        )
        key = jnp.where(hit, before, -1.0)
        valid = ok.astype(f32)
        coded = jnp.where(hit, rel.astype(f32) * (1.0 / PER_BIN) + LIVE + valid * VALID, 0.0)
        slot_id = lax.broadcasted_iota(i32, (n, slots, points), 1).astype(f32)
        chosen = jnp.where(key[:, None, :] == slot_id, coded[:, None, :], 0.0)
        code = jnp.sum(chosen, axis=2, keepdims=True).reshape(n * slots, 1)
        is_valid = code >= VALID
        at_bin = code - jnp.where(is_valid, VALID + LIVE, LIVE)
        weights = jnp.maximum(1.0 - jnp.abs(at_bin - bin_id), 0.0).astype(bf16)
        rows = jnp.dot(weights, table[...], preferred_element_type=f32)
        tiles = rows.reshape(n, slots, width)
        swapped = pltpu.roll(pltpu.roll(tiles, hs, 1), width // 2, 2)
        tiles = jnp.where(stays, tiles, swapped).reshape(hi - lo, SUB, slots, width)
        rows_out[0, lo:hi] = tiles[:, :, 0:hs]
        rows_out[1, lo:hi] = tiles[:, :, hs:slots]
        if k == 0:
            wait_bytes(pair_note, pair_sem)
        for w, h in order[k]:
            give(w, h)
        total_sum += jnp.sum(jnp.where(is_valid, rows, 0.0), axis=0, keepdims=True)
        total_count += jnp.sum(valid, keepdims=True)

    sum_out[0] = total_sum
    near_in[group * SUB + q] = total_sum
    for g, d in [(other_seg, first_at[0] + s) for s in range(SUB)] + [
        (seg, d) for _, d in peers(0)
    ]:
        pltpu.make_async_remote_copy(
            src_ref=sum_out.at[0],
            dst_ref=near_in.at[group * SUB + q],
            send_sem=sum_send.at[0],
            recv_sem=near_sem,
            device_id=(g, d),
            device_id_type=MESH,
        ).start()

    choose(other, pair_note[0:1, :])

    wait_bytes(near_in.at[0 : PAIR * SUB - 1], near_sem)
    near_sum = jnp.sum(near_in[...], axis=0)
    sum_out[1] = near_sum
    far_in[z] = near_sum
    for i in far_first[:-1]:
        pltpu.make_async_remote_copy(
            src_ref=sum_out.at[1],
            dst_ref=far_in.at[z],
            send_sem=sum_send.at[1],
            recv_sem=far_sem,
            device_id=(seg, first_at[i] + q),
            device_id_type=MESH,
        ).start()

    turn = functools.partial(pltpu.roll, shift=width // 2, axis=1)
    hp = points // 2
    for h in range(2):
        both = jnp.zeros((2 * points, width), f32)
        for g in range(PAIR):
            wait_bytes(rows_in.at[h, g], rows_sem.at[h, g])
            got = rows_in[h, g].reshape(n_lat * hs, width)
            high = got.astype(bf16)
            mid = (got - high.astype(f32)).astype(bf16)
            choice = pick[g]
            both += jnp.dot(choice, mid, preferred_element_type=f32)
            both += jnp.dot(choice, high, preferred_element_type=f32)
        part[h, y, 0:hp, :] = jnp.where(
            on_left,
            both[0:hp] + turn(both[points : points + hp]),
            turn(both[hp:points]) + both[points + hp : 2 * points],
        )
        if h == 1:
            wait_bytes(far_in.at[0 : n_z - 1], far_sem)
            part[h, y, hp : hp + 8, :] = jnp.broadcast_to(
                jnp.sum(far_in[...], axis=0), (8, width)
            )
        length = hp + 8 * h

        for peer in y_peers[1:] + y_peers[:1]:
            pltpu.make_async_remote_copy(
                src_ref=part.at[h, y, 0:length],
                dst_ref=part.at[h, y, 0:length],
                send_sem=part_send.at[h],
                recv_sem=part_sem.at[h],
                device_id=(peer, lat),
                device_id_type=MESH,
            ).start()

    sums = []
    for h in range(2):
        length = hp + 8 * h
        wait_bytes(part.at[h, 0 : n_y - 1, 0:length], part_sem.at[h])
        whole = part[h, 0, 0:length]
        for k in range(1, n_y):
            whole = whole + part[h, k, 0:length]
        sums.append(whole)
    left, right_ = sums[0], sums[1][0:hp]
    all_sum = jnp.concatenate(
        [jnp.where(on_left, left, turn(right_)), jnp.where(on_left, turn(left), right_)], axis=0
    )
    valid_total = sums[1][hp : hp + 1]
    stat = all_sum * (1.0 / n_seg)
    stat_ref[...] = stat.astype(bf16)
    global_mean = valid_total * (1.0 / n_seg) / total_count
    row_id = lax.broadcasted_iota(i32, (block_size, width), 0)
    for b in range(blocks):
        count = cnt_ref[b]
        block = stat[b * block_size : (b + 1) * block_size]
        block_sum = jnp.sum(jnp.where(row_id < count, block, 0.0), axis=0, keepdims=True)
        exc_ref[b : b + 1, :] = block_sum / count.astype(f32) - global_mean

    wait_bytes(heard, note_send)
    for h in range(2):
        wait_bytes(rows_in.at[h, 0, 0 : n_lat - 1], rows_send.at[h, 0])
        wait_bytes(rows_in.at[h, 1], rows_send.at[h, 1])
        wait_bytes(part.at[h, 0 : n_y - 1, 0 : hp + 8 * h], part_send.at[h])
    wait_bytes(near_in.at[0 : PAIR * SUB - 1], sum_send.at[0])
    wait_bytes(far_in.at[0 : n_z - 1], sum_send.at[1])


def put_out(stat_ref, exc_ref, stat_out, exc_out, stat_sem, exc_sem):
    stat = pltpu.make_async_copy(stat_ref, stat_out, stat_sem)
    exc = pltpu.make_async_copy(exc_ref, exc_out, exc_sem)
    stat.start()
    exc.start()
    stat.wait()
    exc.wait()


def shards(coh_map, positions, counts):
    n_seg, n_lat = lax.axis_size("seg"), lax.axis_size("lat")
    _, bins, width = coh_map.shape
    points = positions.shape[1]
    blocks = counts.shape[0]
    slots = 2 * points // n_lat
    n_y, n_z = n_seg // PAIR, n_lat // SUB
    dma = pltpu.SemaphoreType.DMA
    vmem = pl.BlockSpec(memory_space=pltpu.VMEM)
    anywhere = pl.BlockSpec(memory_space=pl.ANY)
    stat, excess = pl.pallas_call(
        functools.partial(kernel, n_seg, n_lat),
        out_shape=(
            pltpu.VMEM((points, width), jnp.bfloat16),
            pltpu.VMEM((blocks, width), jnp.float32),
        ),
        in_specs=[
            anywhere,
            anywhere,
            anywhere,
        ],
        out_specs=(vmem, vmem),
        scratch_shapes=[
            pltpu.VMEM((bins, width), jnp.bfloat16),
            pltpu.SMEM((blocks,), jnp.int32),
            pltpu.VMEM((2, points), jnp.int32),
            pltpu.VMEM((n_z, SUB, 2, points), jnp.int32),
            pltpu.VMEM((2, points), jnp.int32),
            pltpu.VMEM((2, n_z, SUB, slots // 2, width), jnp.float32),
            pltpu.VMEM((2, PAIR, n_lat, slots // 2, width), jnp.float32),
            pltpu.VMEM((2, 1, width), jnp.float32),
            pltpu.VMEM((PAIR * SUB, 1, width), jnp.float32),
            pltpu.VMEM((n_z, 1, width), jnp.float32),
            pltpu.VMEM((PAIR, 2 * points, n_lat * slots // 2), jnp.bfloat16),
            pltpu.VMEM((2, n_y, points // 2 + 8, width), jnp.float32),
            dma,
            dma,
            dma,
            dma,
            dma((n_z // 2 + 1,)),
            dma,
            dma((2, 2)),
            dma((2, PAIR)),
            dma((2,)),
            dma,
            dma,
            dma((2,)),
            dma((2,)),
        ],
        compiler_params=pltpu.CompilerParams(collective_id=0, has_side_effects=True),
    )(coh_map, positions, counts)
    in_vmem = functools.partial(pltpu.with_memory_space_constraint, memory_space=pltpu.VMEM)
    return pl.pallas_call(
        put_out,
        out_shape=(
            jax.ShapeDtypeStruct((points, width), jnp.bfloat16),
            jax.ShapeDtypeStruct((blocks, width), jnp.float32),
        ),
        in_specs=[vmem, vmem],
        out_specs=(anywhere, anywhere),
        scratch_shapes=[dma, dma],
    )(in_vmem(stat), in_vmem(excess))


def solution(mesh):
    in_specs = (P("seg", "lat", None), P("seg", "lat"), P("lat"))
    out_specs = (P("lat", None), P("lat", None))
    return jax.shard_map(shards, mesh=mesh, in_specs=in_specs, out_specs=out_specs, check_vma=False)
```

```python
import functools

import jax
import jax.numpy as jnp
from jax import lax
from jax.experimental import pallas as pl
from jax.experimental.pallas import tpu as pltpu
from jax.sharding import PartitionSpec as P

MESH = pl.DeviceIdType.MESH
PER_BIN = 256
SUB = 4
PAIR = 2
LIVE = 4.0
VALID = 4096.0


def wait_bytes(ref, sem):
    pltpu.make_async_copy(ref, ref, sem).wait()


def kernel(
    n_seg,
    n_lat,
    map_ref,
    pos_hbm,
    cnt_hbm,
    stat_ref,
    exc_ref,
    table,
    cnt_ref,
    note,
    heard,
    pair_note,
    rows_out,
    rows_in,
    sum_out,
    near_in,
    mid_in,
    far_in,
    pick,
    part,
    pos_sem,
    cnt_sem,
    table_sem,
    note_send,
    heard_sem,
    pair_sem,
    rows_send,
    rows_sem,
    sum_send,
    near_sem,
    mid_sem,
    far_sem,
    part_send,
    part_sem,
):
    n_y = n_seg // PAIR
    n_z = n_lat // SUB
    half = n_z // 2
    bins, width = table.shape
    points = pos_hbm.shape[1]
    blocks = exc_ref.shape[0]
    block_size = points // blocks
    slots = 2 * points // n_lat
    span = bins * PER_BIN
    f32, bf16, i32 = jnp.float32, jnp.bfloat16, jnp.int32

    seg = lax.axis_index("seg")
    lat = lax.axis_index("lat")
    group, y = lax.div(seg, n_y), lax.rem(seg, n_y)
    other = PAIR - 1 - group
    other_seg = other * n_y + y
    z, q = lax.div(lat, SUB), lax.rem(lat, SUB)

    offsets = [0] + [o for k in range(1, half) for o in (k, n_z - k)] + [half]
    waves = [(0, 1)] + [(2 * k - 1, 2 * k + 1) for k in range(1, half)] + [(n_z - 1, n_z)]
    first_at = [lax.rem(z + o, n_z) * SUB for o in offsets]
    near_q = [lax.rem(q + s, SUB) for s in range(1, SUB)]

    def peers(i):
        if i == 0:
            return [(nq, first_at[0] + nq) for nq in near_q]
        return [(s, first_at[i] + s) for s in (1, 3, 2, 0)]

    y_peers = [group * n_y + k + jnp.where(y <= k, 1, 0) for k in range(n_y - 1)]
    far_first = list(range(n_z - 1, -1, -1))

    load_pos = pltpu.make_async_copy(pos_hbm, note.at[0:1], pos_sem)
    load_cnt = pltpu.make_async_copy(cnt_hbm, cnt_ref, cnt_sem)
    load = pltpu.make_async_copy(map_ref.at[0], table, table_sem)
    load_pos.start()
    load_cnt.start()

    barrier = pltpu.get_barrier_semaphore()
    for i in far_first:
        for _, d in peers(i):
            pl.semaphore_signal(barrier, inc=1, device_id=(seg, d), device_id_type=MESH)
    pl.semaphore_signal(barrier, inc=1, device_id=(other_seg, lat), device_id_type=MESH)
    for peer in y_peers:
        pl.semaphore_signal(barrier, inc=1, device_id=(peer, lat), device_id_type=MESH)

    load.start()

    lane = lax.broadcasted_iota(i32, (1, points), 1)
    limit = jnp.zeros((1, points), i32)
    load_cnt.wait()
    for b in range(blocks):
        limit = jnp.where(lane // block_size == b, cnt_ref[b] + b * block_size, limit)
    note[1:2, :] = jnp.where(lane < limit, 1, 0)

    before_mat = jnp.where(
        lax.broadcasted_iota(i32, (points, points), 0)
        < lax.broadcasted_iota(i32, (points, points), 1),
        1.0,
        0.0,
    ).astype(bf16)
    hs = slots // 2
    dest_id = lax.broadcasted_iota(i32, (n_lat, points), 0)
    flat_id = lax.broadcasted_iota(i32, (n_lat * hs, points), 0).astype(f32)

    def choose(g, positions):
        dest = lax.div(positions, span)
        at_dest = jnp.where(dest == dest_id, 1.0, 0.0)
        ahead = jnp.dot(at_dest.astype(bf16), before_mat, preferred_element_type=f32)
        slot = jnp.sum(at_dest * ahead, axis=0, keepdims=True)
        base = dest.astype(f32) * hs + slot
        flat_low = jnp.where(slot < hs, base, -1.0)
        flat_high = jnp.where(slot < hs, -1.0, base - hs)
        pick[g, 0:points] = jnp.where(flat_id == flat_low, 1.0, 0.0).T.astype(bf16)
        pick[g, points : 2 * points] = jnp.where(flat_id == flat_high, 1.0, 0.0).T.astype(bf16)

    load_pos.wait()
    choose(group, note[0:1, :])

    pl.semaphore_wait(barrier, n_lat - 1 + 1 + n_y - 1)

    for i in far_first:
        w = min(offsets[i], n_z - offsets[i])
        back = offsets.index((n_z - offsets[i]) % n_z)
        for _, d in peers(i):
            pltpu.make_async_remote_copy(
                src_ref=note,
                dst_ref=heard.at[back, q],
                send_sem=note_send,
                recv_sem=heard_sem.at[w],
                device_id=(seg, d),
                device_id_type=MESH,
            ).start()
        if i == n_z - 1:
            pltpu.make_async_remote_copy(
                src_ref=note,
                dst_ref=pair_note,
                send_sem=note_send,
                recv_sem=pair_sem,
                device_id=(other_seg, lat),
                device_id_type=MESH,
            ).start()
    pltpu.make_async_copy(note, heard.at[0, q], heard_sem.at[0]).start()

    def give(i, h):
        if i == 0:
            targets = [(seg, s, d, 0) for s, d in peers(0)]
            targets += [(other_seg, s, first_at[0] + s, 1) for s in range(SUB)]
        else:
            targets = [
                (g * n_y + y, s, d, lax.rem(group + g, PAIR))
                for g in range(PAIR)
                for s, d in peers(i)
            ]
        for to_seg, s, d, which in targets:
            pltpu.make_async_remote_copy(
                src_ref=rows_out.at[h, i, s],
                dst_ref=rows_in.at[h, group, lat],
                send_sem=rows_send.at[h, which],
                recv_sem=rows_sem.at[h, group],
                device_id=(to_seg, d),
                device_id_type=MESH,
            ).start()
        if i == 0:
            pltpu.make_async_copy(
                rows_out.at[h, 0, q], rows_in.at[h, group, lat], rows_sem.at[h, group]
            ).start()

    order = [[], [((1, 2), 0, ""), ((1, 2), 1, "e")], [((3, 4), 0, "")], [((5, 6), 0, "e")], [((7,), 0, "e"), ((5, 6), 0, "l"), ((7,), 0, "l"), ((5, 6, 7), 1, "e"), ((3, 4), 1, "e"), ((5, 6, 7, 3, 4, 1, 2), 1, "l")]]
    early = [first_at[i] < half * SUB for i in range(n_z)]

    tile = (1, slots, width)
    upper = lax.broadcasted_iota(i32, tile, 1) >= hs
    right = lax.broadcasted_iota(i32, tile, 2) >= width // 2
    stays = upper == right
    on_left = lax.broadcasted_iota(i32, (1, width), 1) < width // 2

    load.wait()
    bin_id = lax.broadcasted_iota(i32, (1, bins), 1).astype(f32)
    total_sum = jnp.zeros((1, width), f32)
    total_count = jnp.zeros((1, 1), f32)
    for k, (lo, hi) in enumerate(waves):
        wait_bytes(heard.at[lo:hi], heard_sem.at[k])
        n = (hi - lo) * SUB
        pos = heard[lo:hi, :, 0, :].reshape(n, points)
        ok = heard[lo:hi, :, 1, :].reshape(n, points)
        rel = pos - lat * span
        hit = (rel >= 0) & (rel < span)
        before = jnp.dot(
            jnp.where(hit, 1.0, 0.0).astype(bf16), before_mat, preferred_element_type=f32
        )
        key = jnp.where(hit, before, -1.0)
        valid = ok.astype(f32)
        coded = jnp.where(hit, rel.astype(f32) * (1.0 / PER_BIN) + LIVE + valid * VALID, 0.0)
        slot_id = lax.broadcasted_iota(i32, (n, slots, points), 1).astype(f32)
        chosen = jnp.where(key[:, None, :] == slot_id, coded[:, None, :], 0.0)
        code = jnp.sum(chosen, axis=2, keepdims=True).reshape(n * slots, 1)
        is_valid = code >= VALID
        at_bin = code - jnp.where(is_valid, VALID + LIVE, LIVE)
        weights = jnp.maximum(1.0 - jnp.abs(at_bin - bin_id), 0.0).astype(bf16)
        rows = jnp.dot(weights, table[...], preferred_element_type=f32)
        tiles = rows.reshape(n, slots, width)
        swapped = pltpu.roll(pltpu.roll(tiles, hs, 1), width // 2, 2)
        tiles = jnp.where(stays, tiles, swapped).reshape(hi - lo, SUB, slots, width)
        rows_out[0, lo:hi] = tiles[:, :, 0:hs]
        rows_out[1, lo:hi] = tiles[:, :, hs:slots]
        if k == 0:
            wait_bytes(pair_note, pair_sem)
        total_sum += jnp.sum(jnp.where(is_valid, rows, 0.0), axis=0, keepdims=True)
        total_count += jnp.sum(valid, keepdims=True)

        if k == len(waves) - 1:
            sum_out[0] = total_sum
            near_in[group * SUB + q] = total_sum
            for g, d in [(other_seg, first_at[0] + s) for s in range(SUB)] + [
                (seg, d) for _, d in peers(0)
            ]:
                pltpu.make_async_remote_copy(
                    src_ref=sum_out.at[0],
                    dst_ref=near_in.at[group * SUB + q],
                    send_sem=sum_send.at[0],
                    recv_sem=near_sem,
                    device_id=(g, d),
                    device_id_type=MESH,
                ).start()

        if k == 0:
            give(0, 0)
            give(0, 1)
        for ids, h, cond in order[k]:
            for i in ids:
                if cond == "e":
                    pl.when(early[i])(functools.partial(give, i, h))
                elif cond == "l":
                    pl.when(jnp.logical_not(early[i]))(functools.partial(give, i, h))
                else:
                    give(i, h)

    choose(other, pair_note[0:1, :])

    wait_bytes(near_in.at[0 : PAIR * SUB - 1], near_sem)
    near_sum = jnp.sum(near_in[...], axis=0)
    sum_out[1] = near_sum
    mid_in[z] = near_sum
    for i in range(1, n_z):
        pltpu.make_async_remote_copy(
            src_ref=sum_out.at[1],
            dst_ref=mid_in.at[z],
            send_sem=sum_send.at[1],
            recv_sem=mid_sem,
            device_id=(seg, first_at[i] + q),
            device_id_type=MESH,
        ).start()

    turn = functools.partial(pltpu.roll, shift=width // 2, axis=1)
    hp = points // 2
    for h in range(2):
        both = jnp.zeros((2 * points, width), f32)
        for g in range(PAIR):
            wait_bytes(rows_in.at[h, g], rows_sem.at[h, g])
            got = rows_in[h, g].reshape(n_lat * hs, width)
            high = got.astype(bf16)
            mid = (got - high.astype(f32)).astype(bf16)
            choice = pick[g]
            both += jnp.dot(choice, mid, preferred_element_type=f32)
            both += jnp.dot(choice, high, preferred_element_type=f32)
        part[h, y] = jnp.where(
            on_left,
            both[0:hp] + turn(both[points : points + hp]),
            turn(both[hp:points]) + both[points + hp : 2 * points],
        )

        for peer in y_peers:
            pltpu.make_async_remote_copy(
                src_ref=part.at[h, y],
                dst_ref=part.at[h, y],
                send_sem=part_send.at[h],
                recv_sem=part_sem.at[h],
                device_id=(peer, lat),
                device_id_type=MESH,
            ).start()

        if h == 1:
            wait_bytes(mid_in.at[0 : n_z - 1], mid_sem)
            mid_sum = jnp.sum(mid_in[...], axis=0)
            sum_out[2] = mid_sum
            far_in[y] = mid_sum
            for peer in y_peers:
                pltpu.make_async_remote_copy(
                    src_ref=sum_out.at[2],
                    dst_ref=far_in.at[y],
                    send_sem=sum_send.at[2],
                    recv_sem=far_sem,
                    device_id=(peer, lat),
                    device_id_type=MESH,
                ).start()

    sums = []
    for h in range(2):
        wait_bytes(part.at[h, 0 : n_y - 1], part_sem.at[h])
        whole = part[h, 0]
        for k in range(1, n_y):
            whole = whole + part[h, k]
        sums.append(whole)
    left, right_ = sums[0], sums[1]
    all_sum = jnp.concatenate(
        [jnp.where(on_left, left, turn(right_)), jnp.where(on_left, turn(left), right_)], axis=0
    )
    wait_bytes(far_in.at[0 : n_y - 1], far_sem)
    valid_total = jnp.sum(far_in[...], axis=0)
    stat = all_sum * (1.0 / n_seg)
    stat_ref[...] = stat.astype(bf16)
    global_mean = valid_total * (1.0 / n_seg) / total_count
    row_id = lax.broadcasted_iota(i32, (block_size, width), 0)
    for b in range(blocks):
        count = cnt_ref[b]
        block = stat[b * block_size : (b + 1) * block_size]
        block_sum = jnp.sum(jnp.where(row_id < count, block, 0.0), axis=0, keepdims=True)
        exc_ref[b : b + 1, :] = block_sum / count.astype(f32) - global_mean

    wait_bytes(heard, note_send)
    for h in range(2):
        wait_bytes(rows_in.at[h, 0, 0 : n_lat - 1], rows_send.at[h, 0])
        wait_bytes(rows_in.at[h, 1], rows_send.at[h, 1])
        wait_bytes(part.at[h, 0 : n_y - 1], part_send.at[h])
    wait_bytes(near_in.at[0 : PAIR * SUB - 1], sum_send.at[0])
    wait_bytes(mid_in.at[0 : n_z - 1], sum_send.at[1])
    wait_bytes(far_in.at[0 : n_y - 1], sum_send.at[2])


def put_out(stat_ref, exc_ref, stat_out, exc_out, stat_sem, exc_sem):
    stat = pltpu.make_async_copy(stat_ref, stat_out, stat_sem)
    exc = pltpu.make_async_copy(exc_ref, exc_out, exc_sem)
    stat.start()
    exc.start()
    stat.wait()
    exc.wait()


def shards(coh_map, positions, counts):
    n_seg, n_lat = lax.axis_size("seg"), lax.axis_size("lat")
    _, bins, width = coh_map.shape
    points = positions.shape[1]
    blocks = counts.shape[0]
    slots = 2 * points // n_lat
    n_y, n_z = n_seg // PAIR, n_lat // SUB
    dma = pltpu.SemaphoreType.DMA
    vmem = pl.BlockSpec(memory_space=pltpu.VMEM)
    anywhere = pl.BlockSpec(memory_space=pl.ANY)
    stat, excess = pl.pallas_call(
        functools.partial(kernel, n_seg, n_lat),
        out_shape=(
            pltpu.VMEM((points, width), jnp.bfloat16),
            pltpu.VMEM((blocks, width), jnp.float32),
        ),
        in_specs=[
            anywhere,
            anywhere,
            anywhere,
        ],
        out_specs=(vmem, vmem),
        scratch_shapes=[
            pltpu.VMEM((bins, width), jnp.bfloat16),
            pltpu.SMEM((blocks,), jnp.int32),
            pltpu.VMEM((2, points), jnp.int32),
            pltpu.VMEM((n_z, SUB, 2, points), jnp.int32),
            pltpu.VMEM((2, points), jnp.int32),
            pltpu.VMEM((2, n_z, SUB, slots // 2, width), jnp.float32),
            pltpu.VMEM((2, PAIR, n_lat, slots // 2, width), jnp.float32),
            pltpu.VMEM((3, 1, width), jnp.float32),
            pltpu.VMEM((PAIR * SUB, 1, width), jnp.float32),
            pltpu.VMEM((n_z, 1, width), jnp.float32),
            pltpu.VMEM((n_y, 1, width), jnp.float32),
            pltpu.VMEM((PAIR, 2 * points, n_lat * slots // 2), jnp.bfloat16),
            pltpu.VMEM((2, n_y, points // 2, width), jnp.float32),
            dma,
            dma,
            dma,
            dma,
            dma((n_z // 2 + 1,)),
            dma,
            dma((2, 2)),
            dma((2, PAIR)),
            dma((3,)),
            dma,
            dma,
            dma,
            dma((2,)),
            dma((2,)),
        ],
        compiler_params=pltpu.CompilerParams(collective_id=0, has_side_effects=True),
    )(coh_map, positions, counts)
    in_vmem = functools.partial(pltpu.with_memory_space_constraint, memory_space=pltpu.VMEM)
    return pl.pallas_call(
        put_out,
        out_shape=(
            jax.ShapeDtypeStruct((points, width), jnp.bfloat16),
            jax.ShapeDtypeStruct((blocks, width), jnp.float32),
        ),
        in_specs=[vmem, vmem],
        out_specs=(anywhere, anywhere),
        scratch_shapes=[dma, dma],
    )(in_vmem(stat), in_vmem(excess))


def solution(mesh):
    in_specs = (P("seg", "lat", None), P("seg", "lat"), P("lat"))
    out_specs = (P("lat", None), P("lat", None))
    return jax.shard_map(shards, mesh=mesh, in_specs=in_specs, out_specs=out_specs, check_vma=False)
```

```python
import functools

import jax
import jax.numpy as jnp
from jax import lax
from jax.experimental import pallas as pl
from jax.experimental.pallas import tpu as pltpu
from jax.sharding import PartitionSpec as P

MESH = pl.DeviceIdType.MESH
PER_BIN = 256
SUB = 4
PAIR = 2
LIVE = 4.0
VALID = 4096.0


def wait_bytes(ref, sem):
    pltpu.make_async_copy(ref, ref, sem).wait()


def kernel(
    n_seg,
    n_lat,
    map_ref,
    pos_hbm,
    cnt_hbm,
    stat_ref,
    exc_ref,
    table,
    cnt_ref,
    note,
    heard,
    pair_note,
    rows_out,
    rows_in,
    sum_out,
    near_in,
    mid_in,
    far_in,
    pick,
    part,
    pos_sem,
    cnt_sem,
    table_sem,
    note_send,
    heard_sem,
    pair_sem,
    rows_send,
    rows_sem,
    near_sem,
    mid_sem,
    far_sem,
    part_sem,
):
    n_y = n_seg // PAIR
    n_z = n_lat // SUB
    half = n_z // 2
    bins, width = table.shape
    points = pos_hbm.shape[1]
    blocks = exc_ref.shape[0]
    block_size = points // blocks
    slots = 2 * points // n_lat
    span = bins * PER_BIN
    f32, bf16, i32 = jnp.float32, jnp.bfloat16, jnp.int32

    seg = lax.axis_index("seg")
    lat = lax.axis_index("lat")
    group, y = lax.div(seg, n_y), lax.rem(seg, n_y)
    other = PAIR - 1 - group
    other_seg = other * n_y + y
    z, q = lax.div(lat, SUB), lax.rem(lat, SUB)

    offsets = [0] + [o for k in range(1, half) for o in (k, n_z - k)] + [half]
    waves = [(0, 1)] + [(2 * k - 1, 2 * k + 1) for k in range(1, half)] + [(n_z - 1, n_z)]
    first_at = [lax.rem(z + o, n_z) * SUB for o in offsets]
    near_q = [lax.rem(q + s, SUB) for s in range(1, SUB)]

    def peers(i):
        if i == 0:
            return [(nq, first_at[0] + nq) for nq in near_q]
        return [(s, first_at[i] + s) for s in (1, 3, 2, 0)]

    y_peers = [group * n_y + k + jnp.where(y <= k, 1, 0) for k in range(n_y - 1)]
    far_first = list(range(n_z - 1, -1, -1))

    load_pos = pltpu.make_async_copy(pos_hbm, note.at[0:1], pos_sem)
    load_cnt = pltpu.make_async_copy(cnt_hbm, cnt_ref, cnt_sem)
    load = pltpu.make_async_copy(map_ref.at[0], table, table_sem)
    load_pos.start()
    load_cnt.start()

    barrier = pltpu.get_barrier_semaphore()
    for i in far_first:
        for _, d in peers(i):
            pl.semaphore_signal(barrier, inc=1, device_id=(seg, d), device_id_type=MESH)
    pl.semaphore_signal(barrier, inc=1, device_id=(other_seg, lat), device_id_type=MESH)
    for peer in y_peers:
        pl.semaphore_signal(barrier, inc=1, device_id=(peer, lat), device_id_type=MESH)

    load.start()

    lane = lax.broadcasted_iota(i32, (1, points), 1)
    limit = jnp.zeros((1, points), i32)
    load_cnt.wait()
    for b in range(blocks):
        limit = jnp.where(lane // block_size == b, cnt_ref[b] + b * block_size, limit)
    note[1:2, :] = jnp.where(lane < limit, 1, 0)

    before_mat = jnp.where(
        lax.broadcasted_iota(i32, (points, points), 0)
        < lax.broadcasted_iota(i32, (points, points), 1),
        1.0,
        0.0,
    ).astype(bf16)
    hs = slots // 2
    dest_id = lax.broadcasted_iota(i32, (n_lat, points), 0)
    flat_id = lax.broadcasted_iota(i32, (n_lat * hs, points), 0).astype(f32)

    def choose(g, positions):
        dest = lax.div(positions, span)
        at_dest = jnp.where(dest == dest_id, 1.0, 0.0)
        ahead = jnp.dot(at_dest.astype(bf16), before_mat, preferred_element_type=f32)
        slot = jnp.sum(at_dest * ahead, axis=0, keepdims=True)
        base = dest.astype(f32) * hs + slot
        flat_low = jnp.where(slot < hs, base, -1.0)
        flat_high = jnp.where(slot < hs, -1.0, base - hs)
        depth = n_lat * hs
        for h, flat in enumerate((flat_low, flat_high)):
            choice = jnp.where(flat_id == flat, 1.0, 0.0).T.astype(bf16)
            for c in range(2):
                pick[g, h * points : (h + 1) * points, c * depth : (c + 1) * depth] = choice
        return slot

    load_pos.wait()
    note[2:3, :] = choose(group, note[0:1, :]).astype(i32)

    pl.semaphore_wait(barrier, n_lat - 1 + 1 + n_y - 1)

    for i in far_first:
        w = min(offsets[i], n_z - offsets[i])
        back = offsets.index((n_z - offsets[i]) % n_z)
        for _, d in peers(i):
            pltpu.make_async_remote_copy(
                src_ref=note,
                dst_ref=heard.at[back, q],
                send_sem=note_send,
                recv_sem=heard_sem.at[w],
                device_id=(seg, d),
                device_id_type=MESH,
            ).start()
        if i == n_z - 1:
            pltpu.make_async_remote_copy(
                src_ref=note,
                dst_ref=pair_note,
                send_sem=note_send,
                recv_sem=pair_sem,
                device_id=(other_seg, lat),
                device_id_type=MESH,
            ).start()
    pltpu.make_async_copy(note, heard.at[0, q], heard_sem.at[0]).start()

    def give(i, h):
        if i == 0:
            targets = [(seg, s, d) for s, d in peers(0)]
            targets += [(other_seg, s, first_at[0] + s) for s in range(SUB)]
        else:
            targets = [
                (g * n_y + y, s, d)
                for g in range(PAIR)
                for s, d in peers(i)
            ]
        for to_seg, s, d in targets:
            pltpu.make_async_remote_copy(
                src_ref=rows_out.at[h, i, s],
                dst_ref=rows_in.at[(h * PAIR + group) * n_lat + lat],
                send_sem=rows_send,
                recv_sem=rows_sem.at[h, group],
                device_id=(to_seg, d),
                device_id_type=MESH,
            ).start()
        if i == 0:
            pltpu.make_async_copy(
                rows_out.at[h, 0, q],
                rows_in.at[(h * PAIR + group) * n_lat + lat],
                rows_sem.at[h, group],
            ).start()

    order = [[], [((1, 2), 0, ""), ((1, 2), 1, "e")], [((3, 4), 0, "")], [((5, 6), 0, "e")], [((7,), 0, "e"), ((5, 6, 7), 1, "e"), ((3, 4), 1, "e"), ((5, 6, 7), 0, "l"), ((5, 6, 7, 3, 4, 1, 2), 1, "l")]]
    early = [first_at[i] < half * SUB for i in range(n_z)]

    tile = (1, slots, width)
    upper = lax.broadcasted_iota(i32, tile, 1) >= hs
    right = lax.broadcasted_iota(i32, tile, 2) >= width // 2
    stays = upper == right
    on_left = lax.broadcasted_iota(i32, (1, width), 1) < width // 2

    load.wait()
    bin_id = lax.broadcasted_iota(i32, (1, bins), 1).astype(f32)
    total_sum = jnp.zeros((1, width), f32)
    total_count = jnp.zeros((1, 1), f32)
    for k, (lo, hi) in enumerate(waves):
        wait_bytes(heard.at[lo:hi], heard_sem.at[k])
        n = (hi - lo) * SUB
        pos = heard[lo:hi, :, 0, :].reshape(n, points)
        ok = heard[lo:hi, :, 1, :].reshape(n, points)
        rel = pos - lat * span
        hit = (rel >= 0) & (rel < span)
        rank = heard[lo:hi, :, 2, :].reshape(n, points)
        key = jnp.where(hit, rank.astype(f32), -1.0)
        valid = ok.astype(f32)
        coded = jnp.where(hit, rel.astype(f32) * (1.0 / PER_BIN) + LIVE + valid * VALID, 0.0)
        slot_id = lax.broadcasted_iota(i32, (n, slots, points), 1).astype(f32)
        chosen = jnp.where(key[:, None, :] == slot_id, coded[:, None, :], 0.0)
        code = jnp.sum(chosen, axis=2, keepdims=True).reshape(n * slots, 1)
        is_valid = code >= VALID
        at_bin = code - jnp.where(is_valid, VALID + LIVE, LIVE)
        weights = jnp.maximum(1.0 - jnp.abs(at_bin - bin_id), 0.0).astype(bf16)
        rows = jnp.dot(weights, table[...], preferred_element_type=f32)
        tiles = rows.reshape(n, slots, width)
        swapped = pltpu.roll(pltpu.roll(tiles, hs, 1), width // 2, 2)
        tiles = jnp.where(stays, tiles, swapped).reshape(hi - lo, SUB, slots, width)
        rows_out[0, lo:hi] = tiles[:, :, 0:hs]
        rows_out[1, lo:hi] = tiles[:, :, hs:slots]
        if k == 0:
            wait_bytes(pair_note, pair_sem)
        total_sum += jnp.sum(jnp.where(is_valid, rows, 0.0), axis=0, keepdims=True)
        total_count += jnp.sum(valid, keepdims=True)

        if k == len(waves) - 1:
            sum_out[0] = total_sum
            near_in[group * SUB + q] = total_sum
            for g, d in [(other_seg, first_at[0] + s) for s in range(SUB)] + [
                (seg, d) for _, d in peers(0)
            ]:
                pltpu.make_async_remote_copy(
                    src_ref=sum_out.at[0],
                    dst_ref=near_in.at[group * SUB + q],
                    send_sem=pos_sem,
                    recv_sem=near_sem,
                    device_id=(g, d),
                    device_id_type=MESH,
                ).start()

        if k == 0:
            give(0, 0)
            give(0, 1)
        for ids, h, cond in order[k]:
            for i in ids:
                if cond == "e":
                    pl.when(early[i])(functools.partial(give, i, h))
                elif cond == "l":
                    pl.when(jnp.logical_not(early[i]))(functools.partial(give, i, h))
                else:
                    give(i, h)

    choose(other, pair_note[0:1, :])

    wait_bytes(near_in.at[0 : PAIR * SUB - 1], near_sem)
    near_sum = jnp.sum(near_in[...], axis=0)
    sum_out[1] = near_sum
    mid_in[z] = near_sum
    for i in range(1, n_z):
        pltpu.make_async_remote_copy(
            src_ref=sum_out.at[1],
            dst_ref=mid_in.at[z],
            send_sem=cnt_sem,
            recv_sem=mid_sem,
            device_id=(seg, first_at[i] + q),
            device_id_type=MESH,
        ).start()

    wait_bytes(heard, note_send)
    turn = functools.partial(pltpu.roll, shift=width // 2, axis=1)
    hp = points // 2
    for h in range(2):
        both = jnp.zeros((2 * points, width), f32)
        for g in range(PAIR):
            lo = (h * PAIR + g) * n_lat
            wait_bytes(rows_in.at[lo : lo + n_lat], rows_sem.at[h, g])
            got = rows_in[lo : lo + n_lat].reshape(n_lat * hs, width)
            high = got.astype(bf16)
            mid = (got - high.astype(f32)).astype(bf16)
            terms = jnp.concatenate([high, mid], axis=0)
            both += jnp.dot(pick[g], terms, preferred_element_type=f32)
        part[h * n_y + y] = jnp.where(
            on_left,
            both[0:hp] + turn(both[points : points + hp]),
            turn(both[hp:points]) + both[points + hp : 2 * points],
        )

        for peer in y_peers:
            pltpu.make_async_remote_copy(
                src_ref=part.at[h * n_y + y],
                dst_ref=part.at[h * n_y + y],
                send_sem=note_send,
                recv_sem=part_sem.at[h],
                device_id=(peer, lat),
                device_id_type=MESH,
            ).start()

        if h == 1:
            wait_bytes(mid_in.at[0 : n_z - 1], mid_sem)
            mid_sum = jnp.sum(mid_in[...], axis=0)
            sum_out[2] = mid_sum
            far_in[y] = mid_sum
            for peer in y_peers:
                pltpu.make_async_remote_copy(
                    src_ref=sum_out.at[2],
                    dst_ref=far_in.at[y],
                    send_sem=table_sem,
                    recv_sem=far_sem,
                    device_id=(peer, lat),
                    device_id_type=MESH,
                ).start()

    wait_bytes(rows_in.at[0 : 2 * (PAIR * n_lat - 1)], rows_send)
    wait_bytes(near_in.at[0 : PAIR * SUB - 1], pos_sem)
    wait_bytes(mid_in.at[0 : n_z - 1], cnt_sem)
    wait_bytes(far_in.at[0 : n_y - 1], table_sem)

    sums = []
    for h in range(2):
        wait_bytes(part.at[0 : n_y - 1], part_sem.at[h])
        whole = part[h * n_y]
        for k in range(1, n_y):
            whole = whole + part[h * n_y + k]
        sums.append(whole)
    left, right_ = sums[0], sums[1]
    all_sum = jnp.concatenate(
        [jnp.where(on_left, left, turn(right_)), jnp.where(on_left, turn(left), right_)], axis=0
    )
    wait_bytes(far_in.at[0 : n_y - 1], far_sem)
    valid_total = jnp.sum(far_in[...], axis=0)
    stat = all_sum * (1.0 / n_seg)
    stat_ref[...] = stat.astype(bf16)
    global_mean = valid_total * (1.0 / n_seg) / total_count
    row_id = lax.broadcasted_iota(i32, (block_size, width), 0)
    for b in range(blocks):
        count = cnt_ref[b]
        block = stat[b * block_size : (b + 1) * block_size]
        block_sum = jnp.sum(jnp.where(row_id < count, block, 0.0), axis=0, keepdims=True)
        exc_ref[b : b + 1, :] = block_sum / count.astype(f32) - global_mean

    wait_bytes(part.at[0 : 2 * (n_y - 1)], note_send)


def put_out(stat_ref, exc_ref, stat_out, exc_out, stat_sem, exc_sem):
    stat = pltpu.make_async_copy(stat_ref, stat_out, stat_sem)
    exc = pltpu.make_async_copy(exc_ref, exc_out, exc_sem)
    stat.start()
    exc.start()
    stat.wait()
    exc.wait()


def shards(coh_map, positions, counts):
    n_seg, n_lat = lax.axis_size("seg"), lax.axis_size("lat")
    _, bins, width = coh_map.shape
    points = positions.shape[1]
    blocks = counts.shape[0]
    slots = 2 * points // n_lat
    n_y, n_z = n_seg // PAIR, n_lat // SUB
    dma = pltpu.SemaphoreType.DMA
    vmem = pl.BlockSpec(memory_space=pltpu.VMEM)
    anywhere = pl.BlockSpec(memory_space=pl.ANY)
    stat, excess = pl.pallas_call(
        functools.partial(kernel, n_seg, n_lat),
        out_shape=(
            pltpu.VMEM((points, width), jnp.bfloat16),
            pltpu.VMEM((blocks, width), jnp.float32),
        ),
        in_specs=[
            anywhere,
            anywhere,
            anywhere,
        ],
        out_specs=(vmem, vmem),
        scratch_shapes=[
            pltpu.VMEM((bins, width), jnp.bfloat16),
            pltpu.SMEM((blocks,), jnp.int32),
            pltpu.VMEM((3, points), jnp.int32),
            pltpu.VMEM((n_z, SUB, 3, points), jnp.int32),
            pltpu.VMEM((3, points), jnp.int32),
            pltpu.VMEM((2, n_z, SUB, slots // 2, width), jnp.float32),
            pltpu.VMEM((2 * PAIR * n_lat, slots // 2, width), jnp.float32),
            pltpu.VMEM((3, 1, width), jnp.float32),
            pltpu.VMEM((PAIR * SUB, 1, width), jnp.float32),
            pltpu.VMEM((n_z, 1, width), jnp.float32),
            pltpu.VMEM((n_y, 1, width), jnp.float32),
            pltpu.VMEM((PAIR, 2 * points, n_lat * slots), jnp.bfloat16),
            pltpu.VMEM((2 * n_y, points // 2, width), jnp.float32),
            dma,
            dma,
            dma,
            dma,
            dma((n_z // 2 + 1,)),
            dma,
            dma,
            dma((2, PAIR)),
            dma,
            dma,
            dma,
            dma((2,)),
        ],
        compiler_params=pltpu.CompilerParams(collective_id=0, has_side_effects=True),
    )(coh_map, positions, counts)
    in_vmem = functools.partial(pltpu.with_memory_space_constraint, memory_space=pltpu.VMEM)
    return pl.pallas_call(
        put_out,
        out_shape=(
            jax.ShapeDtypeStruct((points, width), jnp.bfloat16),
            jax.ShapeDtypeStruct((blocks, width), jnp.float32),
        ),
        in_specs=[vmem, vmem],
        out_specs=(anywhere, anywhere),
        scratch_shapes=[dma, dma],
    )(in_vmem(stat), in_vmem(excess))


def solution(mesh):
    in_specs = (P("seg", "lat", None), P("seg", "lat"), P("lat"))
    out_specs = (P("lat", None), P("lat", None))
    return jax.shard_map(shards, mesh=mesh, in_specs=in_specs, out_specs=out_specs, check_vma=False)
```

```python
import functools

import jax
import jax.numpy as jnp
from jax import lax
from jax.experimental import pallas as pl
from jax.experimental.pallas import tpu as pltpu
from jax.sharding import PartitionSpec as P

MESH = pl.DeviceIdType.MESH
PER_BIN = 256
SUB = 4
PAIR = 2
LIVE = 4.0
VALID = 4096.0


def wait_bytes(ref, sem):
    pltpu.make_async_copy(ref, ref, sem).wait()


def kernel(
    n_seg,
    n_lat,
    map_ref,
    pos_hbm,
    cnt_hbm,
    stat_ref,
    exc_ref,
    table,
    cnt_ref,
    note,
    heard,
    pair_note,
    rows_out,
    rows_in,
    sum_out,
    near_in,
    mid_in,
    far_in,
    pick,
    part,
    pos_sem,
    cnt_sem,
    table_sem,
    note_send,
    heard_sem,
    pair_sem,
    rows_send,
    rows_sem,
    near_sem,
    mid_sem,
    far_sem,
    part_sem,
):
    n_y = n_seg // PAIR
    n_z = n_lat // SUB
    half = n_z // 2
    bins, width = table.shape
    points = pos_hbm.shape[1]
    blocks = exc_ref.shape[0]
    block_size = points // blocks
    slots = 2 * points // n_lat
    span = bins * PER_BIN
    f32, bf16, i32 = jnp.float32, jnp.bfloat16, jnp.int32

    seg = lax.axis_index("seg")
    lat = lax.axis_index("lat")
    group, y = lax.div(seg, n_y), lax.rem(seg, n_y)
    other = PAIR - 1 - group
    other_seg = other * n_y + y
    z, q = lax.div(lat, SUB), lax.rem(lat, SUB)

    offsets = [0] + [o for k in range(1, half) for o in (k, n_z - k)] + [half]
    waves = [(0, 1)] + [(2 * k - 1, 2 * k + 1) for k in range(1, half)] + [(n_z - 1, n_z)]
    first_at = [lax.rem(z + o, n_z) * SUB for o in offsets]
    near_q = [lax.rem(q + s, SUB) for s in range(1, SUB)]

    def peers(i):
        if i == 0:
            return [(nq, first_at[0] + nq) for nq in near_q]
        return [(s, first_at[i] + s) for s in (1, 3, 2, 0)]

    y_peers = [group * n_y + k + jnp.where(y <= k, 1, 0) for k in range(n_y - 1)]
    far_first = list(range(n_z - 1, -1, -1))

    load_pos = pltpu.make_async_copy(pos_hbm, note.at[0:1], pos_sem)
    load_cnt = pltpu.make_async_copy(cnt_hbm, cnt_ref, cnt_sem)
    load = pltpu.make_async_copy(map_ref.at[0], table, table_sem)
    load_pos.start()
    load_cnt.start()

    barrier = pltpu.get_barrier_semaphore()
    for i in far_first:
        for _, d in peers(i):
            pl.semaphore_signal(barrier, inc=1, device_id=(seg, d), device_id_type=MESH)
    pl.semaphore_signal(barrier, inc=1, device_id=(other_seg, lat), device_id_type=MESH)
    for peer in y_peers:
        pl.semaphore_signal(barrier, inc=1, device_id=(peer, lat), device_id_type=MESH)

    load.start()

    lane = lax.broadcasted_iota(i32, (1, points), 1)
    limit = jnp.zeros((1, points), i32)
    load_cnt.wait()
    for b in range(blocks):
        limit = jnp.where(lane // block_size == b, cnt_ref[b] + b * block_size, limit)
    note[1:2, :] = jnp.where(lane < limit, 1, 0)

    before_mat = jnp.where(
        lax.broadcasted_iota(i32, (points, points), 0)
        < lax.broadcasted_iota(i32, (points, points), 1),
        1.0,
        0.0,
    ).astype(bf16)
    hs = slots // 2
    dest_id = lax.broadcasted_iota(i32, (n_lat, points), 0)
    flat_id = lax.broadcasted_iota(i32, (n_lat * hs, points), 0).astype(f32)

    def choose(g, positions):
        dest = lax.div(positions, span)
        at_dest = jnp.where(dest == dest_id, 1.0, 0.0)
        ahead = jnp.dot(at_dest.astype(bf16), before_mat, preferred_element_type=f32)
        slot = jnp.sum(at_dest * ahead, axis=0, keepdims=True)
        base = dest.astype(f32) * hs + slot
        flat_low = jnp.where(slot < hs, base, -1.0)
        flat_high = jnp.where(slot < hs, -1.0, base - hs)
        depth = n_lat * hs
        for h, flat in enumerate((flat_low, flat_high)):
            choice = jnp.where(flat_id == flat, 1.0, 0.0).T.astype(bf16)
            for c in range(2):
                pick[g, h * points : (h + 1) * points, c * depth : (c + 1) * depth] = choice
        return slot

    load_pos.wait()
    note[2:3, :] = choose(group, note[0:1, :]).astype(i32)

    pl.semaphore_wait(barrier, n_lat - 1 + 1 + n_y - 1)

    for i in far_first:
        w = min(offsets[i], n_z - offsets[i])
        back = offsets.index((n_z - offsets[i]) % n_z)
        for _, d in peers(i):
            pltpu.make_async_remote_copy(
                src_ref=note,
                dst_ref=heard.at[back, q],
                send_sem=note_send,
                recv_sem=heard_sem.at[w],
                device_id=(seg, d),
                device_id_type=MESH,
            ).start()
        if i == n_z - 1:
            pltpu.make_async_remote_copy(
                src_ref=note,
                dst_ref=pair_note,
                send_sem=note_send,
                recv_sem=pair_sem,
                device_id=(other_seg, lat),
                device_id_type=MESH,
            ).start()
    pltpu.make_async_copy(note, heard.at[0, q], heard_sem.at[0]).start()

    def give(i, h):
        if i == 0:
            targets = [(seg, s, d) for s, d in peers(0)]
            targets += [(other_seg, s, first_at[0] + s) for s in range(SUB)]
        else:
            targets = [
                (g * n_y + y, s, d)
                for g in range(PAIR)
                for s, d in peers(i)
            ]
        for to_seg, s, d in targets:
            pltpu.make_async_remote_copy(
                src_ref=rows_out.at[h, i, s],
                dst_ref=rows_in.at[(h * PAIR + group) * n_lat + lat],
                send_sem=rows_send,
                recv_sem=rows_sem.at[h, group],
                device_id=(to_seg, d),
                device_id_type=MESH,
            ).start()
        if i == 0:
            pltpu.make_async_copy(
                rows_out.at[h, 0, q],
                rows_in.at[(h * PAIR + group) * n_lat + lat],
                rows_sem.at[h, group],
            ).start()

    order = [[], [((1, 2), 0, ""), ((1, 2), 1, "e")], [((3, 4), 0, "")], [((5, 6), 0, "e")], [((7,), 0, "e"), ((7, 5, 6), 1, "e"), ((3, 4), 1, "e"), ((7, 5, 6), 0, "l"), ((7, 5, 6, 3, 4, 1, 2), 1, "l")]]
    early = [first_at[i] < half * SUB for i in range(n_z)]

    tile = (1, slots, width)
    upper = lax.broadcasted_iota(i32, tile, 1) >= hs
    right = lax.broadcasted_iota(i32, tile, 2) >= width // 2
    stays = upper == right
    on_left = lax.broadcasted_iota(i32, (1, width), 1) < width // 2

    load.wait()
    bin_id = lax.broadcasted_iota(i32, (1, bins), 1).astype(f32)
    total_sum = jnp.zeros((1, width), f32)
    total_count = jnp.zeros((1, 1), f32)
    for k, (lo, hi) in enumerate(waves):
        wait_bytes(heard.at[lo:hi], heard_sem.at[k])
        n = (hi - lo) * SUB
        pos = heard[lo:hi, :, 0, :].reshape(n, points)
        ok = heard[lo:hi, :, 1, :].reshape(n, points)
        rel = pos - lat * span
        hit = (rel >= 0) & (rel < span)
        rank = heard[lo:hi, :, 2, :].reshape(n, points)
        key = jnp.where(hit, rank.astype(f32), -1.0)
        valid = ok.astype(f32)
        coded = jnp.where(hit, rel.astype(f32) * (1.0 / PER_BIN) + LIVE + valid * VALID, 0.0)
        slot_id = lax.broadcasted_iota(i32, (n, slots, points), 1).astype(f32)
        chosen = jnp.where(key[:, None, :] == slot_id, coded[:, None, :], 0.0)
        code = jnp.sum(chosen, axis=2, keepdims=True).reshape(n * slots, 1)
        is_valid = code >= VALID
        at_bin = code - jnp.where(is_valid, VALID + LIVE, LIVE)
        weights = jnp.maximum(1.0 - jnp.abs(at_bin - bin_id), 0.0).astype(bf16)
        rows = jnp.dot(weights, table[...], preferred_element_type=f32)
        tiles = rows.reshape(n, slots, width)
        swapped = pltpu.roll(pltpu.roll(tiles, hs, 1), width // 2, 2)
        tiles = jnp.where(stays, tiles, swapped).reshape(hi - lo, SUB, slots, width)
        rows_out[0, lo:hi] = tiles[:, :, 0:hs]
        rows_out[1, lo:hi] = tiles[:, :, hs:slots]
        if k == 0:
            wait_bytes(pair_note, pair_sem)
        total_sum += jnp.sum(jnp.where(is_valid, rows, 0.0), axis=0, keepdims=True)
        total_count += jnp.sum(valid, keepdims=True)

        if k == 0:
            give(0, 0)
            give(0, 1)
        for ids, h, cond in order[k]:
            for i in ids:
                if cond == "e":
                    pl.when(early[i])(functools.partial(give, i, h))
                elif cond == "l":
                    pl.when(jnp.logical_not(early[i]))(functools.partial(give, i, h))
                else:
                    give(i, h)

        if k == len(waves) - 1:
            sum_out[0] = total_sum
            near_in[group * SUB + q] = total_sum
            for g, d in [(other_seg, first_at[0] + s) for s in range(SUB)] + [
                (seg, d) for _, d in peers(0)
            ]:
                pltpu.make_async_remote_copy(
                    src_ref=sum_out.at[0],
                    dst_ref=near_in.at[group * SUB + q],
                    send_sem=pos_sem,
                    recv_sem=near_sem,
                    device_id=(g, d),
                    device_id_type=MESH,
                ).start()

    choose(other, pair_note[0:1, :])

    wait_bytes(near_in.at[0 : PAIR * SUB - 1], near_sem)
    near_sum = jnp.sum(near_in[...], axis=0)
    sum_out[1] = near_sum
    mid_in[z] = near_sum
    for i in range(1, n_z):
        pltpu.make_async_remote_copy(
            src_ref=sum_out.at[1],
            dst_ref=mid_in.at[z],
            send_sem=cnt_sem,
            recv_sem=mid_sem,
            device_id=(seg, first_at[i] + q),
            device_id_type=MESH,
        ).start()

    wait_bytes(heard, note_send)
    turn = functools.partial(pltpu.roll, shift=width // 2, axis=1)
    hp = points // 2
    for h in range(2):
        both = jnp.zeros((2 * points, width), f32)
        for g in range(PAIR):
            lo = (h * PAIR + g) * n_lat
            wait_bytes(rows_in.at[lo : lo + n_lat], rows_sem.at[h, g])
            got = rows_in[lo : lo + n_lat].reshape(n_lat * hs, width)
            high = got.astype(bf16)
            mid = (got - high.astype(f32)).astype(bf16)
            terms = jnp.concatenate([high, mid], axis=0)
            both += jnp.dot(pick[g], terms, preferred_element_type=f32)
        part[h * n_y + y] = jnp.where(
            on_left,
            both[0:hp] + turn(both[points : points + hp]),
            turn(both[hp:points]) + both[points + hp : 2 * points],
        )

        for peer in y_peers:
            pltpu.make_async_remote_copy(
                src_ref=part.at[h * n_y + y],
                dst_ref=part.at[h * n_y + y],
                send_sem=note_send,
                recv_sem=part_sem.at[h],
                device_id=(peer, lat),
                device_id_type=MESH,
            ).start()

        if h == 1:
            wait_bytes(mid_in.at[0 : n_z - 1], mid_sem)
            mid_sum = jnp.sum(mid_in[...], axis=0)
            sum_out[2] = mid_sum
            far_in[y] = mid_sum
            for peer in y_peers:
                pltpu.make_async_remote_copy(
                    src_ref=sum_out.at[2],
                    dst_ref=far_in.at[y],
                    send_sem=table_sem,
                    recv_sem=far_sem,
                    device_id=(peer, lat),
                    device_id_type=MESH,
                ).start()

    wait_bytes(rows_in.at[0 : 2 * (PAIR * n_lat - 1)], rows_send)
    wait_bytes(near_in.at[0 : PAIR * SUB - 1], pos_sem)
    wait_bytes(mid_in.at[0 : n_z - 1], cnt_sem)
    wait_bytes(far_in.at[0 : n_y - 1], table_sem)

    sums = []
    for h in range(2):
        wait_bytes(part.at[0 : n_y - 1], part_sem.at[h])
        whole = part[h * n_y]
        for k in range(1, n_y):
            whole = whole + part[h * n_y + k]
        sums.append(whole)
    left, right_ = sums[0], sums[1]
    all_sum = jnp.concatenate(
        [jnp.where(on_left, left, turn(right_)), jnp.where(on_left, turn(left), right_)], axis=0
    )
    wait_bytes(far_in.at[0 : n_y - 1], far_sem)
    valid_total = jnp.sum(far_in[...], axis=0)
    stat = all_sum * (1.0 / n_seg)
    stat_ref[...] = stat.astype(bf16)
    global_mean = valid_total * (1.0 / n_seg) / total_count
    row_id = lax.broadcasted_iota(i32, (block_size, width), 0)
    for b in range(blocks):
        count = cnt_ref[b]
        block = stat[b * block_size : (b + 1) * block_size]
        block_sum = jnp.sum(jnp.where(row_id < count, block, 0.0), axis=0, keepdims=True)
        exc_ref[b : b + 1, :] = block_sum / count.astype(f32) - global_mean

    wait_bytes(part.at[0 : 2 * (n_y - 1)], note_send)


def put_out(stat_ref, exc_ref, stat_out, exc_out, stat_sem, exc_sem):
    stat = pltpu.make_async_copy(stat_ref, stat_out, stat_sem)
    exc = pltpu.make_async_copy(exc_ref, exc_out, exc_sem)
    stat.start()
    exc.start()
    stat.wait()
    exc.wait()


def shards(coh_map, positions, counts):
    n_seg, n_lat = lax.axis_size("seg"), lax.axis_size("lat")
    _, bins, width = coh_map.shape
    points = positions.shape[1]
    blocks = counts.shape[0]
    slots = 2 * points // n_lat
    n_y, n_z = n_seg // PAIR, n_lat // SUB
    dma = pltpu.SemaphoreType.DMA
    vmem = pl.BlockSpec(memory_space=pltpu.VMEM)
    anywhere = pl.BlockSpec(memory_space=pl.ANY)
    stat, excess = pl.pallas_call(
        functools.partial(kernel, n_seg, n_lat),
        out_shape=(
            pltpu.VMEM((points, width), jnp.bfloat16),
            pltpu.VMEM((blocks, width), jnp.float32),
        ),
        in_specs=[
            anywhere,
            anywhere,
            anywhere,
        ],
        out_specs=(vmem, vmem),
        scratch_shapes=[
            pltpu.VMEM((bins, width), jnp.bfloat16),
            pltpu.SMEM((blocks,), jnp.int32),
            pltpu.VMEM((3, points), jnp.int32),
            pltpu.VMEM((n_z, SUB, 3, points), jnp.int32),
            pltpu.VMEM((3, points), jnp.int32),
            pltpu.VMEM((2, n_z, SUB, slots // 2, width), jnp.float32),
            pltpu.VMEM((2 * PAIR * n_lat, slots // 2, width), jnp.float32),
            pltpu.VMEM((3, 1, width), jnp.float32),
            pltpu.VMEM((PAIR * SUB, 1, width), jnp.float32),
            pltpu.VMEM((n_z, 1, width), jnp.float32),
            pltpu.VMEM((n_y, 1, width), jnp.float32),
            pltpu.VMEM((PAIR, 2 * points, n_lat * slots), jnp.bfloat16),
            pltpu.VMEM((2 * n_y, points // 2, width), jnp.float32),
            dma,
            dma,
            dma,
            dma,
            dma((n_z // 2 + 1,)),
            dma,
            dma,
            dma((2, PAIR)),
            dma,
            dma,
            dma,
            dma((2,)),
        ],
        compiler_params=pltpu.CompilerParams(collective_id=0, has_side_effects=True),
    )(coh_map, positions, counts)
    in_vmem = functools.partial(pltpu.with_memory_space_constraint, memory_space=pltpu.VMEM)
    return pl.pallas_call(
        put_out,
        out_shape=(
            jax.ShapeDtypeStruct((points, width), jnp.bfloat16),
            jax.ShapeDtypeStruct((blocks, width), jnp.float32),
        ),
        in_specs=[vmem, vmem],
        out_specs=(anywhere, anywhere),
        scratch_shapes=[dma, dma],
    )(in_vmem(stat), in_vmem(excess))


def solution(mesh):
    in_specs = (P("seg", "lat", None), P("seg", "lat"), P("lat"))
    out_specs = (P("lat", None), P("lat", None))
    return jax.shard_map(shards, mesh=mesh, in_specs=in_specs, out_specs=out_specs, check_vma=False)
```

```python
import functools

import jax
import jax.numpy as jnp
from jax import lax
from jax.experimental import pallas as pl
from jax.experimental.pallas import tpu as pltpu
from jax.sharding import PartitionSpec as P

MESH = pl.DeviceIdType.MESH
PER_BIN = 256
SUB = 4
PAIR = 2
LIVE = 4.0
VALID = 4096.0


def wait_bytes(ref, sem):
    pltpu.make_async_copy(ref, ref, sem).wait()


def kernel(
    n_seg,
    n_lat,
    map_ref,
    pos_hbm,
    cnt_hbm,
    stat_ref,
    exc_ref,
    table,
    cnt_ref,
    note,
    heard,
    pair_note,
    rows_out,
    rows_in,
    sum_out,
    near_in,
    mid_in,
    far_in,
    pick,
    part,
    pos_sem,
    cnt_sem,
    table_sem,
    note_send,
    heard_sem,
    pair_sem,
    rows_send,
    rows_sem,
    near_sem,
    mid_sem,
    far_sem,
    part_sem,
):
    n_y = n_seg // PAIR
    n_z = n_lat // SUB
    half = n_z // 2
    bins, width = table.shape
    points = pos_hbm.shape[1]
    blocks = exc_ref.shape[0]
    block_size = points // blocks
    slots = 2 * points // n_lat
    span = bins * PER_BIN
    f32, bf16, i32 = jnp.float32, jnp.bfloat16, jnp.int32

    seg = lax.axis_index("seg")
    lat = lax.axis_index("lat")
    group, y = lax.div(seg, n_y), lax.rem(seg, n_y)
    other = PAIR - 1 - group
    other_seg = other * n_y + y
    z, q = lax.div(lat, SUB), lax.rem(lat, SUB)

    offsets = [0] + [o for k in range(1, half) for o in (k, n_z - k)] + [half]
    waves = [(0, 1)] + [(2 * k - 1, 2 * k + 1) for k in range(1, half)] + [(n_z - 1, n_z)]
    first_at = [lat - q + (o - jnp.where(z >= n_z - o, n_z, 0)) * SUB for o in offsets]
    near_q = [q + s - jnp.where(q >= SUB - s, SUB, 0) for s in range(1, SUB)]

    def peers(i):
        if i == 0:
            return [(nq, first_at[0] + nq) for nq in near_q]
        return [(s, first_at[i] + s) for s in (1, 3, 2, 0)]

    y_peers = [group * n_y + k + jnp.where(y <= k, 1, 0) for k in range(n_y - 1)]
    far_first = list(range(n_z - 1, -1, -1))

    load_pos = pltpu.make_async_copy(pos_hbm, note.at[0:1], pos_sem)
    load_cnt = pltpu.make_async_copy(cnt_hbm, cnt_ref, cnt_sem)
    load = pltpu.make_async_copy(map_ref.at[0], table, table_sem)
    load_pos.start()
    load_cnt.start()

    barrier = pltpu.get_barrier_semaphore()
    for i in far_first:
        for _, d in peers(i):
            pl.semaphore_signal(barrier, inc=1, device_id=(seg, d), device_id_type=MESH)
    pl.semaphore_signal(barrier, inc=1, device_id=(other_seg, lat), device_id_type=MESH)
    for peer in y_peers:
        pl.semaphore_signal(barrier, inc=1, device_id=(peer, lat), device_id_type=MESH)

    load.start()

    lane = lax.broadcasted_iota(i32, (1, points), 1)
    limit = jnp.zeros((1, points), i32)
    load_cnt.wait()
    for b in range(blocks):
        limit = jnp.where(lane // block_size == b, cnt_ref[b] + b * block_size, limit)
    note[1:2, :] = jnp.where(lane < limit, 1, 0)

    before_mat = jnp.where(
        lax.broadcasted_iota(i32, (points, points), 0)
        < lax.broadcasted_iota(i32, (points, points), 1),
        1.0,
        0.0,
    ).astype(bf16)
    hs = slots // 2
    dest_id = lax.broadcasted_iota(i32, (n_lat, points), 0)
    flat_id = lax.broadcasted_iota(i32, (n_lat * hs, points), 0).astype(f32)

    def choose(g, positions):
        dest = lax.div(positions, span)
        at_dest = jnp.where(dest == dest_id, 1.0, 0.0)
        ahead = jnp.dot(at_dest.astype(bf16), before_mat, preferred_element_type=f32)
        slot = jnp.sum(at_dest * ahead, axis=0, keepdims=True)
        base = dest.astype(f32) * hs + slot
        flat_low = jnp.where(slot < hs, base, -1.0)
        flat_high = jnp.where(slot < hs, -1.0, base - hs)
        depth = n_lat * hs
        for h, flat in enumerate((flat_low, flat_high)):
            choice = jnp.where(flat_id == flat, 1.0, 0.0).T.astype(bf16)
            for c in range(2):
                pick[g, h * points : (h + 1) * points, c * depth : (c + 1) * depth] = choice
        return slot

    load_pos.wait()
    note[2:3, :] = choose(group, note[0:1, :]).astype(i32)

    pl.semaphore_wait(barrier, n_lat - 1 + 1 + n_y - 1)

    for i in far_first:
        w = min(offsets[i], n_z - offsets[i])
        back = offsets.index((n_z - offsets[i]) % n_z)
        for _, d in peers(i):
            pltpu.make_async_remote_copy(
                src_ref=note,
                dst_ref=heard.at[back, q],
                send_sem=note_send,
                recv_sem=heard_sem.at[w],
                device_id=(seg, d),
                device_id_type=MESH,
            ).start()
        if i == n_z - 1:
            pltpu.make_async_remote_copy(
                src_ref=note,
                dst_ref=pair_note,
                send_sem=note_send,
                recv_sem=pair_sem,
                device_id=(other_seg, lat),
                device_id_type=MESH,
            ).start()
    pltpu.make_async_copy(note, heard.at[0, q], heard_sem.at[0]).start()

    def give(i, h):
        if i == 0:
            targets = [(seg, s, d) for s, d in peers(0)]
            targets += [(other_seg, s, first_at[0] + s) for s in range(SUB)]
        else:
            targets = [
                (g * n_y + y, s, d)
                for g in range(PAIR)
                for s, d in peers(i)
            ]
        for to_seg, s, d in targets:
            pltpu.make_async_remote_copy(
                src_ref=rows_out.at[h, i, s],
                dst_ref=rows_in.at[(h * PAIR + group) * n_lat + lat],
                send_sem=rows_send,
                recv_sem=rows_sem.at[h, group],
                device_id=(to_seg, d),
                device_id_type=MESH,
            ).start()
        if i == 0:
            pltpu.make_async_copy(
                rows_out.at[h, 0, q],
                rows_in.at[(h * PAIR + group) * n_lat + lat],
                rows_sem.at[h, group],
            ).start()

    order = [[], [((1, 2), 0, ""), ((1, 2), 1, "e")], [((3, 4), 0, "")], [((5, 6), 0, "e")], [((7,), 0, "e"), ((7, 5, 6), 1, "e"), ((3, 4), 1, "e"), ((7, 5, 6), 0, "l"), ((7, 5, 6, 3, 4, 1, 2), 1, "l")]]
    early = [first_at[i] < half * SUB for i in range(n_z)]

    tile = (1, slots, width)
    upper = lax.broadcasted_iota(i32, tile, 1) >= hs
    right = lax.broadcasted_iota(i32, tile, 2) >= width // 2
    stays = upper == right
    on_left = lax.broadcasted_iota(i32, (1, width), 1) < width // 2

    load.wait()
    bin_id = lax.broadcasted_iota(i32, (1, bins), 1).astype(f32)
    total_sum = jnp.zeros((1, width), f32)
    total_count = jnp.zeros((1, 1), f32)
    for k, (lo, hi) in enumerate(waves):
        wait_bytes(heard.at[lo:hi], heard_sem.at[k])
        n = (hi - lo) * SUB
        pos = heard[lo:hi, :, 0, :].reshape(n, points)
        ok = heard[lo:hi, :, 1, :].reshape(n, points)
        rel = pos - lat * span
        hit = (rel >= 0) & (rel < span)
        rank = heard[lo:hi, :, 2, :].reshape(n, points)
        key = jnp.where(hit, rank.astype(f32), -1.0)
        valid = ok.astype(f32)
        coded = jnp.where(hit, rel.astype(f32) * (1.0 / PER_BIN) + LIVE + valid * VALID, 0.0)
        slot_id = lax.broadcasted_iota(i32, (n, slots, points), 1).astype(f32)
        chosen = jnp.where(key[:, None, :] == slot_id, coded[:, None, :], 0.0)
        code = jnp.sum(chosen, axis=2, keepdims=True).reshape(n * slots, 1)
        is_valid = code >= VALID
        at_bin = code - jnp.where(is_valid, VALID + LIVE, LIVE)
        weights = jnp.maximum(1.0 - jnp.abs(at_bin - bin_id), 0.0).astype(bf16)
        rows = jnp.dot(weights, table[...], preferred_element_type=f32)
        tiles = rows.reshape(n, slots, width)
        swapped = pltpu.roll(pltpu.roll(tiles, hs, 1), width // 2, 2)
        tiles = jnp.where(stays, tiles, swapped).reshape(hi - lo, SUB, slots, width)
        rows_out[0, lo:hi] = tiles[:, :, 0:hs]
        rows_out[1, lo:hi] = tiles[:, :, hs:slots]
        if k == 0:
            wait_bytes(pair_note, pair_sem)
        total_sum += jnp.sum(jnp.where(is_valid, rows, 0.0), axis=0, keepdims=True)
        total_count += jnp.sum(valid, keepdims=True)

        if k == 0:
            give(0, 0)
            give(0, 1)
        for ids, h, cond in order[k]:
            for i in ids:
                if cond == "e":
                    pl.when(early[i])(functools.partial(give, i, h))
                elif cond == "l":
                    pl.when(jnp.logical_not(early[i]))(functools.partial(give, i, h))
                else:
                    give(i, h)

        if k == len(waves) - 1:
            sum_out[0] = total_sum
            near_in[group * SUB + q] = total_sum
            for g, d in [(other_seg, first_at[0] + s) for s in range(SUB)] + [
                (seg, d) for _, d in peers(0)
            ]:
                pltpu.make_async_remote_copy(
                    src_ref=sum_out.at[0],
                    dst_ref=near_in.at[group * SUB + q],
                    send_sem=pos_sem,
                    recv_sem=near_sem,
                    device_id=(g, d),
                    device_id_type=MESH,
                ).start()

    choose(other, pair_note[0:1, :])

    wait_bytes(near_in.at[0 : PAIR * SUB - 1], near_sem)
    near_sum = jnp.sum(near_in[...], axis=0)
    sum_out[1] = near_sum
    mid_in[z] = near_sum
    for i in range(1, n_z):
        pltpu.make_async_remote_copy(
            src_ref=sum_out.at[1],
            dst_ref=mid_in.at[z],
            send_sem=cnt_sem,
            recv_sem=mid_sem,
            device_id=(seg, first_at[i] + q),
            device_id_type=MESH,
        ).start()

    wait_bytes(heard, note_send)
    turn = functools.partial(pltpu.roll, shift=width // 2, axis=1)
    hp = points // 2
    for h in range(2):
        both = jnp.zeros((2 * points, width), f32)
        for g in range(PAIR):
            lo = (h * PAIR + g) * n_lat
            wait_bytes(rows_in.at[lo : lo + n_lat], rows_sem.at[h, g])
            got = rows_in[lo : lo + n_lat].reshape(n_lat * hs, width)
            high = got.astype(bf16)
            mid = (got - high.astype(f32)).astype(bf16)
            terms = jnp.concatenate([high, mid], axis=0)
            both += jnp.dot(pick[g], terms, preferred_element_type=f32)
        part[h * n_y + y] = jnp.where(
            on_left,
            both[0:hp] + turn(both[points : points + hp]),
            turn(both[hp:points]) + both[points + hp : 2 * points],
        )

        for peer in y_peers:
            pltpu.make_async_remote_copy(
                src_ref=part.at[h * n_y + y],
                dst_ref=part.at[h * n_y + y],
                send_sem=note_send,
                recv_sem=part_sem.at[h],
                device_id=(peer, lat),
                device_id_type=MESH,
            ).start()

        if h == 1:
            wait_bytes(mid_in.at[0 : n_z - 1], mid_sem)
            mid_sum = jnp.sum(mid_in[...], axis=0)
            sum_out[2] = mid_sum
            far_in[y] = mid_sum
            for peer in y_peers:
                pltpu.make_async_remote_copy(
                    src_ref=sum_out.at[2],
                    dst_ref=far_in.at[y],
                    send_sem=table_sem,
                    recv_sem=far_sem,
                    device_id=(peer, lat),
                    device_id_type=MESH,
                ).start()

    wait_bytes(rows_in.at[0 : 2 * (PAIR * n_lat - 1)], rows_send)
    wait_bytes(near_in.at[0 : PAIR * SUB - 1], pos_sem)
    wait_bytes(mid_in.at[0 : n_z - 1], cnt_sem)
    wait_bytes(far_in.at[0 : n_y - 1], table_sem)

    sums = []
    for h in range(2):
        wait_bytes(part.at[0 : n_y - 1], part_sem.at[h])
        whole = part[h * n_y]
        for k in range(1, n_y):
            whole = whole + part[h * n_y + k]
        sums.append(whole)
    left, right_ = sums[0], sums[1]
    all_sum = jnp.concatenate(
        [jnp.where(on_left, left, turn(right_)), jnp.where(on_left, turn(left), right_)], axis=0
    )
    wait_bytes(far_in.at[0 : n_y - 1], far_sem)
    valid_total = jnp.sum(far_in[...], axis=0)
    stat = all_sum * (1.0 / n_seg)
    stat_ref[...] = stat.astype(bf16)
    global_mean = valid_total * (1.0 / n_seg) / total_count
    row_id = lax.broadcasted_iota(i32, (block_size, width), 0)
    for b in range(blocks):
        count = cnt_ref[b]
        block = stat[b * block_size : (b + 1) * block_size]
        block_sum = jnp.sum(jnp.where(row_id < count, block, 0.0), axis=0, keepdims=True)
        exc_ref[b : b + 1, :] = block_sum / count.astype(f32) - global_mean

    wait_bytes(part.at[0 : 2 * (n_y - 1)], note_send)


def put_out(stat_ref, exc_ref, stat_out, exc_out, stat_sem, exc_sem):
    stat = pltpu.make_async_copy(stat_ref, stat_out, stat_sem)
    exc = pltpu.make_async_copy(exc_ref, exc_out, exc_sem)
    stat.start()
    exc.start()
    stat.wait()
    exc.wait()


def shards(coh_map, positions, counts):
    n_seg, n_lat = lax.axis_size("seg"), lax.axis_size("lat")
    _, bins, width = coh_map.shape
    points = positions.shape[1]
    blocks = counts.shape[0]
    slots = 2 * points // n_lat
    n_y, n_z = n_seg // PAIR, n_lat // SUB
    dma = pltpu.SemaphoreType.DMA
    vmem = pl.BlockSpec(memory_space=pltpu.VMEM)
    anywhere = pl.BlockSpec(memory_space=pl.ANY)
    stat, excess = pl.pallas_call(
        functools.partial(kernel, n_seg, n_lat),
        out_shape=(
            pltpu.VMEM((points, width), jnp.bfloat16),
            pltpu.VMEM((blocks, width), jnp.float32),
        ),
        in_specs=[
            anywhere,
            anywhere,
            anywhere,
        ],
        out_specs=(vmem, vmem),
        scratch_shapes=[
            pltpu.VMEM((bins, width), jnp.bfloat16),
            pltpu.SMEM((blocks,), jnp.int32),
            pltpu.VMEM((3, points), jnp.int32),
            pltpu.VMEM((n_z, SUB, 3, points), jnp.int32),
            pltpu.VMEM((3, points), jnp.int32),
            pltpu.VMEM((2, n_z, SUB, slots // 2, width), jnp.float32),
            pltpu.VMEM((2 * PAIR * n_lat, slots // 2, width), jnp.float32),
            pltpu.VMEM((3, 1, width), jnp.float32),
            pltpu.VMEM((PAIR * SUB, 1, width), jnp.float32),
            pltpu.VMEM((n_z, 1, width), jnp.float32),
            pltpu.VMEM((n_y, 1, width), jnp.float32),
            pltpu.VMEM((PAIR, 2 * points, n_lat * slots), jnp.bfloat16),
            pltpu.VMEM((2 * n_y, points // 2, width), jnp.float32),
            dma,
            dma,
            dma,
            dma,
            dma((n_z // 2 + 1,)),
            dma,
            dma,
            dma((2, PAIR)),
            dma,
            dma,
            dma,
            dma((2,)),
        ],
        compiler_params=pltpu.CompilerParams(collective_id=0, has_side_effects=True),
    )(coh_map, positions, counts)
    in_vmem = functools.partial(pltpu.with_memory_space_constraint, memory_space=pltpu.VMEM)
    return pl.pallas_call(
        put_out,
        out_shape=(
            jax.ShapeDtypeStruct((points, width), jnp.bfloat16),
            jax.ShapeDtypeStruct((blocks, width), jnp.float32),
        ),
        in_specs=[vmem, vmem],
        out_specs=(anywhere, anywhere),
        scratch_shapes=[dma, dma],
    )(in_vmem(stat), in_vmem(excess))


def solution(mesh):
    in_specs = (P("seg", "lat", None), P("seg", "lat"), P("lat"))
    out_specs = (P("lat", None), P("lat", None))
    return jax.shard_map(shards, mesh=mesh, in_specs=in_specs, out_specs=out_specs, check_vma=False)
```

```python
import functools

import jax
import jax.numpy as jnp
from jax import lax
from jax.experimental import pallas as pl
from jax.experimental.pallas import tpu as pltpu
from jax.sharding import PartitionSpec as P

MESH = pl.DeviceIdType.MESH
PER_BIN = 256
SUB = 4
PAIR = 2
LIVE = 4.0
VALID = 4096.0


def wait_bytes(ref, sem):
    pltpu.make_async_copy(ref, ref, sem).wait()


def kernel(
    n_seg,
    n_lat,
    map_ref,
    pos_hbm,
    cnt_hbm,
    stat_ref,
    exc_ref,
    table,
    cnt_ref,
    note,
    heard,
    pair_note,
    rows_out,
    rows_in,
    sum_out,
    near_in,
    mid_in,
    far_in,
    pick,
    part,
    pos_sem,
    cnt_sem,
    table_sem,
    note_send,
    heard_sem,
    pair_sem,
    rows_send,
    rows_sem,
    near_sem,
    mid_sem,
    far_sem,
    part_sem,
):
    n_y = n_seg // PAIR
    n_z = n_lat // SUB
    half = n_z // 2
    bins, width = table.shape
    points = pos_hbm.shape[1]
    blocks = exc_ref.shape[0]
    block_size = points // blocks
    slots = 2 * points // n_lat
    span = bins * PER_BIN
    f32, bf16, i32 = jnp.float32, jnp.bfloat16, jnp.int32

    seg = lax.axis_index("seg")
    lat = lax.axis_index("lat")
    group, y = lax.div(seg, n_y), lax.rem(seg, n_y)
    other = PAIR - 1 - group
    other_seg = other * n_y + y
    z, q = lax.div(lat, SUB), lax.rem(lat, SUB)

    offsets = [0] + [o for k in range(1, half) for o in (k, n_z - k)] + [half]
    waves = [(0, 1)] + [(2 * k - 1, 2 * k + 1) for k in range(1, half)] + [(n_z - 1, n_z)]
    first_at = [lat - q + (o - jnp.where(z >= n_z - o, n_z, 0)) * SUB for o in offsets]
    near_q = [q + s - jnp.where(q >= SUB - s, SUB, 0) for s in range(1, SUB)]

    def peers(i):
        if i == 0:
            return [(nq, first_at[0] + nq) for nq in near_q]
        return [(s, first_at[i] + s) for s in (1, 0, 3, 2)]

    y_peers = [group * n_y + k + jnp.where(y <= k, 1, 0) for k in range(n_y - 1)]
    far_first = list(range(n_z - 1, -1, -1))

    load_pos = pltpu.make_async_copy(pos_hbm, note.at[0:1], pos_sem)
    load_cnt = pltpu.make_async_copy(cnt_hbm, cnt_ref, cnt_sem)
    load = pltpu.make_async_copy(map_ref.at[0], table, table_sem)
    load_pos.start()
    load_cnt.start()

    barrier = pltpu.get_barrier_semaphore()
    for i in far_first:
        for _, d in peers(i):
            pl.semaphore_signal(barrier, inc=1, device_id=(seg, d), device_id_type=MESH)
    pl.semaphore_signal(barrier, inc=1, device_id=(other_seg, lat), device_id_type=MESH)
    for peer in y_peers:
        pl.semaphore_signal(barrier, inc=1, device_id=(peer, lat), device_id_type=MESH)

    load.start()

    lane = lax.broadcasted_iota(i32, (1, points), 1)
    limit = jnp.zeros((1, points), i32)
    load_cnt.wait()
    for b in range(blocks):
        limit = jnp.where(lane // block_size == b, cnt_ref[b] + b * block_size, limit)
    note[1:2, :] = jnp.where(lane < limit, 1, 0)

    before_mat = jnp.where(
        lax.broadcasted_iota(i32, (points, points), 0)
        < lax.broadcasted_iota(i32, (points, points), 1),
        1.0,
        0.0,
    ).astype(bf16)
    hs = slots // 2
    dest_id = lax.broadcasted_iota(i32, (n_lat, points), 0)
    flat_id = lax.broadcasted_iota(i32, (n_lat * hs, points), 0).astype(f32)

    def choose(g, positions):
        dest = lax.div(positions, span)
        at_dest = jnp.where(dest == dest_id, 1.0, 0.0)
        ahead = jnp.dot(at_dest.astype(bf16), before_mat, preferred_element_type=f32)
        slot = jnp.sum(at_dest * ahead, axis=0, keepdims=True)
        base = dest.astype(f32) * hs + slot
        flat_low = jnp.where(slot < hs, base, -1.0)
        flat_high = jnp.where(slot < hs, -1.0, base - hs)
        depth = n_lat * hs
        for h, flat in enumerate((flat_low, flat_high)):
            choice = jnp.where(flat_id == flat, 1.0, 0.0).T.astype(bf16)
            for c in range(2):
                pick[g, h * points : (h + 1) * points, c * depth : (c + 1) * depth] = choice
        return slot

    load_pos.wait()
    note[2:3, :] = choose(group, note[0:1, :]).astype(i32)

    pl.semaphore_wait(barrier, n_lat - 1 + 1 + n_y - 1)

    for i in far_first:
        w = min(offsets[i], n_z - offsets[i])
        back = offsets.index((n_z - offsets[i]) % n_z)
        for _, d in peers(i):
            pltpu.make_async_remote_copy(
                src_ref=note,
                dst_ref=heard.at[back, q],
                send_sem=note_send,
                recv_sem=heard_sem.at[w],
                device_id=(seg, d),
                device_id_type=MESH,
            ).start()
        if i == n_z - 1:
            pltpu.make_async_remote_copy(
                src_ref=note,
                dst_ref=pair_note,
                send_sem=note_send,
                recv_sem=pair_sem,
                device_id=(other_seg, lat),
                device_id_type=MESH,
            ).start()
    pltpu.make_async_copy(note, heard.at[0, q], heard_sem.at[0]).start()

    def give(i, h):
        if i == 0:
            targets = [(seg, s, d) for s, d in peers(0)]
            targets += [(other_seg, s, first_at[0] + s) for s in range(SUB)]
        else:
            targets = [
                (g * n_y + y, s, d)
                for g in range(PAIR)
                for s, d in peers(i)
            ]
        for to_seg, s, d in targets:
            pltpu.make_async_remote_copy(
                src_ref=rows_out.at[h, i, s],
                dst_ref=rows_in.at[(h * PAIR + group) * n_lat + lat],
                send_sem=rows_send,
                recv_sem=rows_sem.at[h, group],
                device_id=(to_seg, d),
                device_id_type=MESH,
            ).start()
        if i == 0:
            pltpu.make_async_copy(
                rows_out.at[h, 0, q],
                rows_in.at[(h * PAIR + group) * n_lat + lat],
                rows_sem.at[h, group],
            ).start()

    order = [[], [((1, 2), 0, ""), ((1, 2), 1, "e")], [((3, 4), 0, "")], [((5, 6), 0, "e")], [((7,), 0, "e"), ((7, 5, 6), 1, "e"), ((3, 4), 1, "e"), ((7, 5, 6), 0, "l"), ((7, 5, 6, 3, 4, 1, 2), 1, "l")]]
    early = [first_at[i] < half * SUB for i in range(n_z)]

    tile = (1, slots, width)
    upper = lax.broadcasted_iota(i32, tile, 1) >= hs
    right = lax.broadcasted_iota(i32, tile, 2) >= width // 2
    stays = upper == right
    on_left = lax.broadcasted_iota(i32, (1, width), 1) < width // 2

    load.wait()
    bin_id = lax.broadcasted_iota(i32, (1, bins), 1).astype(f32)
    total_sum = jnp.zeros((1, width), f32)
    total_count = jnp.zeros((1, 1), f32)
    for k, (lo, hi) in enumerate(waves):
        wait_bytes(heard.at[lo:hi], heard_sem.at[k])
        n = (hi - lo) * SUB
        pos = heard[lo:hi, :, 0, :].reshape(n, points)
        ok = heard[lo:hi, :, 1, :].reshape(n, points)
        rel = pos - lat * span
        hit = (rel >= 0) & (rel < span)
        rank = heard[lo:hi, :, 2, :].reshape(n, points)
        key = jnp.where(hit, rank.astype(f32), -1.0)
        valid = ok.astype(f32)
        coded = jnp.where(hit, rel.astype(f32) * (1.0 / PER_BIN) + LIVE + valid * VALID, 0.0)
        slot_id = lax.broadcasted_iota(i32, (n, slots, points), 1).astype(f32)
        chosen = jnp.where(key[:, None, :] == slot_id, coded[:, None, :], 0.0)
        code = jnp.sum(chosen, axis=2, keepdims=True).reshape(n * slots, 1)
        is_valid = code >= VALID
        at_bin = code - jnp.where(is_valid, VALID + LIVE, LIVE)
        weights = jnp.maximum(1.0 - jnp.abs(at_bin - bin_id), 0.0).astype(bf16)
        rows = jnp.dot(weights, table[...], preferred_element_type=f32)
        tiles = rows.reshape(n, slots, width)
        swapped = pltpu.roll(pltpu.roll(tiles, hs, 1), width // 2, 2)
        tiles = jnp.where(stays, tiles, swapped).reshape(hi - lo, SUB, slots, width)
        rows_out[0, lo:hi] = tiles[:, :, 0:hs]
        rows_out[1, lo:hi] = tiles[:, :, hs:slots]
        if k == 0:
            wait_bytes(pair_note, pair_sem)
        total_sum += jnp.sum(jnp.where(is_valid, rows, 0.0), axis=0, keepdims=True)
        total_count += jnp.sum(valid, keepdims=True)

        if k == 0:
            give(0, 0)
            give(0, 1)
        for ids, h, cond in order[k]:
            for i in ids:
                if cond == "e":
                    pl.when(early[i])(functools.partial(give, i, h))
                elif cond == "l":
                    pl.when(jnp.logical_not(early[i]))(functools.partial(give, i, h))
                else:
                    give(i, h)

        if k == len(waves) - 1:
            sum_out[0] = total_sum
            near_in[group * SUB + q] = total_sum
            for g, d in [(other_seg, first_at[0] + s) for s in range(SUB)] + [
                (seg, d) for _, d in peers(0)
            ]:
                pltpu.make_async_remote_copy(
                    src_ref=sum_out.at[0],
                    dst_ref=near_in.at[group * SUB + q],
                    send_sem=pos_sem,
                    recv_sem=near_sem,
                    device_id=(g, d),
                    device_id_type=MESH,
                ).start()

    choose(other, pair_note[0:1, :])

    wait_bytes(near_in.at[0 : PAIR * SUB - 1], near_sem)
    near_sum = jnp.sum(near_in[...], axis=0)
    sum_out[1] = near_sum
    mid_in[z] = near_sum
    for i in range(1, n_z):
        pltpu.make_async_remote_copy(
            src_ref=sum_out.at[1],
            dst_ref=mid_in.at[z],
            send_sem=cnt_sem,
            recv_sem=mid_sem,
            device_id=(seg, first_at[i] + q),
            device_id_type=MESH,
        ).start()

    wait_bytes(heard, note_send)
    turn = functools.partial(pltpu.roll, shift=width // 2, axis=1)
    hp = points // 2
    for h in range(2):
        both = jnp.zeros((2 * points, width), f32)
        for g in range(PAIR):
            lo = (h * PAIR + g) * n_lat
            wait_bytes(rows_in.at[lo : lo + n_lat], rows_sem.at[h, g])
            got = rows_in[lo : lo + n_lat].reshape(n_lat * hs, width)
            high = got.astype(bf16)
            mid = (got - high.astype(f32)).astype(bf16)
            terms = jnp.concatenate([high, mid], axis=0)
            both += jnp.dot(pick[g], terms, preferred_element_type=f32)
        part[h * n_y + y] = jnp.where(
            on_left,
            both[0:hp] + turn(both[points : points + hp]),
            turn(both[hp:points]) + both[points + hp : 2 * points],
        )

        for peer in y_peers:
            pltpu.make_async_remote_copy(
                src_ref=part.at[h * n_y + y],
                dst_ref=part.at[h * n_y + y],
                send_sem=note_send,
                recv_sem=part_sem.at[h],
                device_id=(peer, lat),
                device_id_type=MESH,
            ).start()

        if h == 1:
            wait_bytes(mid_in.at[0 : n_z - 1], mid_sem)
            mid_sum = jnp.sum(mid_in[...], axis=0)
            sum_out[2] = mid_sum
            far_in[y] = mid_sum
            for peer in y_peers:
                pltpu.make_async_remote_copy(
                    src_ref=sum_out.at[2],
                    dst_ref=far_in.at[y],
                    send_sem=table_sem,
                    recv_sem=far_sem,
                    device_id=(peer, lat),
                    device_id_type=MESH,
                ).start()

    wait_bytes(rows_in.at[0 : 2 * (PAIR * n_lat - 1)], rows_send)
    wait_bytes(near_in.at[0 : PAIR * SUB - 1], pos_sem)
    wait_bytes(mid_in.at[0 : n_z - 1], cnt_sem)
    wait_bytes(far_in.at[0 : n_y - 1], table_sem)

    sums = []
    for h in range(2):
        wait_bytes(part.at[0 : n_y - 1], part_sem.at[h])
        whole = part[h * n_y]
        for k in range(1, n_y):
            whole = whole + part[h * n_y + k]
        sums.append(whole)
    left, right_ = sums[0], sums[1]
    all_sum = jnp.concatenate(
        [jnp.where(on_left, left, turn(right_)), jnp.where(on_left, turn(left), right_)], axis=0
    )
    wait_bytes(far_in.at[0 : n_y - 1], far_sem)
    valid_total = jnp.sum(far_in[...], axis=0)
    stat = all_sum * (1.0 / n_seg)
    stat_ref[...] = stat.astype(bf16)
    global_mean = valid_total * (1.0 / n_seg) / total_count
    row_id = lax.broadcasted_iota(i32, (block_size, width), 0)
    for b in range(blocks):
        count = cnt_ref[b]
        block = stat[b * block_size : (b + 1) * block_size]
        block_sum = jnp.sum(jnp.where(row_id < count, block, 0.0), axis=0, keepdims=True)
        exc_ref[b : b + 1, :] = block_sum / count.astype(f32) - global_mean

    wait_bytes(part.at[0 : 2 * (n_y - 1)], note_send)


def put_out(stat_ref, exc_ref, stat_out, exc_out, stat_sem, exc_sem):
    stat = pltpu.make_async_copy(stat_ref, stat_out, stat_sem)
    exc = pltpu.make_async_copy(exc_ref, exc_out, exc_sem)
    stat.start()
    exc.start()
    stat.wait()
    exc.wait()


def shards(coh_map, positions, counts):
    n_seg, n_lat = lax.axis_size("seg"), lax.axis_size("lat")
    _, bins, width = coh_map.shape
    points = positions.shape[1]
    blocks = counts.shape[0]
    slots = 2 * points // n_lat
    n_y, n_z = n_seg // PAIR, n_lat // SUB
    dma = pltpu.SemaphoreType.DMA
    vmem = pl.BlockSpec(memory_space=pltpu.VMEM)
    anywhere = pl.BlockSpec(memory_space=pl.ANY)
    stat, excess = pl.pallas_call(
        functools.partial(kernel, n_seg, n_lat),
        out_shape=(
            pltpu.VMEM((points, width), jnp.bfloat16),
            pltpu.VMEM((blocks, width), jnp.float32),
        ),
        in_specs=[
            anywhere,
            anywhere,
            anywhere,
        ],
        out_specs=(vmem, vmem),
        scratch_shapes=[
            pltpu.VMEM((bins, width), jnp.bfloat16),
            pltpu.SMEM((blocks,), jnp.int32),
            pltpu.VMEM((3, points), jnp.int32),
            pltpu.VMEM((n_z, SUB, 3, points), jnp.int32),
            pltpu.VMEM((3, points), jnp.int32),
            pltpu.VMEM((2, n_z, SUB, slots // 2, width), jnp.float32),
            pltpu.VMEM((2 * PAIR * n_lat, slots // 2, width), jnp.float32),
            pltpu.VMEM((3, 1, width), jnp.float32),
            pltpu.VMEM((PAIR * SUB, 1, width), jnp.float32),
            pltpu.VMEM((n_z, 1, width), jnp.float32),
            pltpu.VMEM((n_y, 1, width), jnp.float32),
            pltpu.VMEM((PAIR, 2 * points, n_lat * slots), jnp.bfloat16),
            pltpu.VMEM((2 * n_y, points // 2, width), jnp.float32),
            dma,
            dma,
            dma,
            dma,
            dma((n_z // 2 + 1,)),
            dma,
            dma,
            dma((2, PAIR)),
            dma,
            dma,
            dma,
            dma((2,)),
        ],
        compiler_params=pltpu.CompilerParams(collective_id=0, has_side_effects=True),
    )(coh_map, positions, counts)
    in_vmem = functools.partial(pltpu.with_memory_space_constraint, memory_space=pltpu.VMEM)
    return pl.pallas_call(
        put_out,
        out_shape=(
            jax.ShapeDtypeStruct((points, width), jnp.bfloat16),
            jax.ShapeDtypeStruct((blocks, width), jnp.float32),
        ),
        in_specs=[vmem, vmem],
        out_specs=(anywhere, anywhere),
        scratch_shapes=[dma, dma],
    )(in_vmem(stat), in_vmem(excess))


def solution(mesh):
    in_specs = (P("seg", "lat", None), P("seg", "lat"), P("lat"))
    out_specs = (P("lat", None), P("lat", None))
    return jax.shard_map(shards, mesh=mesh, in_specs=in_specs, out_specs=out_specs, check_vma=False)
```
